32 devices in a mesh: row: 4 (over x, core), col: 8 (over z, y).
Axes of the slice: x: 2, y: 2, z: 4, core: 2. Of those that a mesh axis runs over, the one named last changes fastest.
Arguments:
- right_sides: bfloat16 [1024, 64, 128], P(('row', 'col')), may hold values from -7 to 7
- weights_fine: bfloat16 [1024, 3, 128, 128], P(('row', 'col')), may hold values from 0 to 2
- columns_fine: int32 [1024, 3], P(('row', 'col')), may hold values from 0 to 1023, as said below
- degree_fine: float32 [1024, 128], P(('row', 'col')), may hold values from 0.05 to 0.5
- owners_fine: int32 [1024, 128], P(('row', 'col')), may hold values from 0 to 31, as said below
- slots_fine: int32 [1024, 128], P(('row', 'col')), may hold values from 0 to 1023
- weights_second: bfloat16 [256, 3, 128, 128], P(('row', 'col')), may hold values from 0 to 8
- columns_second: int32 [256, 3], P(('row', 'col')), may hold values from 0 to 255, as said below
- degree_second: float32 [256, 128], P(('row', 'col')), may hold values from 0.2 to 2
- owners_second: int32 [256, 128], P(('row', 'col')), may hold values from 0 to 31, as said below
- slots_second: int32 [256, 128], P(('row', 'col')), may hold values from 0 to 255
- weights_third: bfloat16 [64, 3, 128, 128], P(('row', 'col')), may hold values from 0 to 32
- columns_third: int32 [64, 3], P(('row', 'col')), may hold values from 0 to 63, as said below
- degree_third: float32 [64, 128], P(('row', 'col')), may hold values from 0.8 to 8
- owners_third: int32 [64, 128], P(('row', 'col')), may hold values from 0 to 31, as said below
- slots_third: int32 [64, 128], P(('row', 'col')), may hold values from 0 to 127
- coarse_inverse: bfloat16 [4096, 1024], P(('row', 'col')), may hold values from -1 to 1, as said below
Outputs:
- solution: float32 [1024, 64, 128], P(('row', 'col'))
The draws below stay inside these ranges and needn't reach their ends.
Inputs may be any that keep to these rules, and one draw needn't show every extreme that they name: `columns_fine`: every entry lies within 2 blocks of its own row block's index, on the same level. `columns_second`: every entry lies within 2 blocks of its own row block's index, on the same level. `columns_third`: every entry lies within 2 blocks of its own row block's index, on the same level. `owners_fine`: each entry is the device holding the vertex or the one just before or after it in device order. `owners_second`: each entry is the device holding the vertex or the one just before or after it in device order. `owners_third`: each entry is the device holding the vertex or the one just before or after it in device order. `coarse_inverse`: each row group's block is symmetric.
All inputs are finite; a program needn't handle non-finite values.
Results may differ from the reference program's by a relative error of at most 0.0003.
Values may be sent and summed in bfloat16 or wider, within the bound.
A program may use at most 64 MiB of HBM per device.

```python
import math
import jax
import jax.numpy as jnp
from jax import lax

RHS_COUNT = 64
BS = 128
K = 3
HB = 2
SWEEPS = 2
NB2 = 2
NB1 = 8
NB0 = 32
C3 = 128
M3 = 1024
N_ROW = 4
DEVICES = 32


def arrange_columns(drawn, blocks_here):
    total = blocks_here * DEVICES
    spread = 2 * HB + 1
    scores = drawn * spread + jnp.arange(spread, dtype=jnp.int32)[None, :]
    chosen = jnp.argsort(scores, axis=1)[:, :K].astype(jnp.int32) - HB
    rows_here = jnp.arange(total, dtype=jnp.int32)[:, None]
    target = rows_here + chosen
    outside = (target < 0) | (target >= total)
    return jnp.where(outside, rows_here - chosen, target).astype(jnp.int32)


def arrange_owners(drawn, blocks_here):
    total = blocks_here * DEVICES
    device = (jnp.arange(total, dtype=jnp.int32) // blocks_here)[:, None]
    moved = jnp.where(drawn == 6, -1, jnp.where(drawn == 7, 1, 0))
    return jnp.clip(device + moved, 0, DEVICES - 1).astype(jnp.int32)


def draw_right_sides(key, part):
    total_blocks = NB0 * DEVICES
    vertex = (jnp.arange(total_blocks, dtype=jnp.float32)[:, None, None] * BS + jnp.arange(BS, dtype=jnp.float32)[None, None, :]) / (total_blocks * BS * 1.0)
    frequency = jax.random.randint(jax.random.fold_in(key, 41), (RHS_COUNT,), 1, 4).astype(jnp.float32)
    phase = jax.random.uniform(jax.random.fold_in(key, 42), (RHS_COUNT,), jnp.float32, -3.14159, 3.14159)
    amplitude = jax.random.uniform(jax.random.fold_in(key, 43), (RHS_COUNT,), jnp.float32, 0.25, 0.5)
    wave = jnp.sin(6.283185 * frequency[None, :, None] * vertex + phase[None, :, None])
    shape = (total_blocks, RHS_COUNT, BS)
    flips = jax.random.randint(jax.random.fold_in(key, 45), (RHS_COUNT,), 0, 2)
    signs = jnp.where(flips == 0, -1.0, 1.0).astype(jnp.float32)
    smooth = (signs * amplitude)[None, :, None] * wave
    rough = jnp.clip(jax.random.normal(jax.random.fold_in(key, 44), shape, jnp.float32), -6.0, 6.0)
    return (smooth + rough).astype(jnp.bfloat16)


def draw_columns_fine(key, part):
    drawn = jax.random.randint(jax.random.fold_in(key, 11), (NB0 * DEVICES, 2 * HB + 1), 0, 1 << 20)
    return arrange_columns(drawn, NB0)


def draw_columns_second(key, part):
    drawn = jax.random.randint(jax.random.fold_in(key, 12), (NB1 * DEVICES, 2 * HB + 1), 0, 1 << 20)
    return arrange_columns(drawn, NB1)


def draw_columns_third(key, part):
    drawn = jax.random.randint(jax.random.fold_in(key, 13), (NB2 * DEVICES, 2 * HB + 1), 0, 1 << 20)
    return arrange_columns(drawn, NB2)


def draw_owners_fine(key, part):
    drawn = jax.random.randint(jax.random.fold_in(key, 21), (NB0 * DEVICES, BS), 0, 8)
    return arrange_owners(drawn, NB0)


def draw_owners_second(key, part):
    drawn = jax.random.randint(jax.random.fold_in(key, 22), (NB1 * DEVICES, BS), 0, 8)
    return arrange_owners(drawn, NB1)


def draw_owners_third(key, part):
    drawn = jax.random.randint(jax.random.fold_in(key, 23), (NB2 * DEVICES, BS), 0, 8)
    return arrange_owners(drawn, NB2)


def draw_coarse_inverse(key, part):
    groups = DEVICES * C3 // M3
    inner = jax.random.fold_in(key, 31)
    raw = jnp.clip(jax.random.normal(inner, (groups, M3, M3), jnp.float32), -3.0, 3.0)
    symmetric = 0.5 * (raw + jnp.transpose(raw, (0, 2, 1))) * (0.025 / jnp.sqrt(M3 * 1.0))
    matrix = symmetric + 0.05 * jnp.eye(M3, dtype=jnp.float32)[None, :, :]
    return matrix.reshape(groups * M3, M3).astype(jnp.bfloat16)


def place_ends(values, rng, smallest, top_value):
    extent = values.shape
    index_at = [jax.random.randint(jax.random.fold_in(rng, axis), (), 0, extent[axis]) for axis in range(len(extent))]
    values = values.at[tuple(index_at)].set(smallest)
    longest = extent.index(max(extent))
    index_at[longest] = (index_at[longest] + 1) % extent[longest]
    return values.at[tuple(index_at)].set(top_value)


def block_levels(key, extent, pieces, least, largest):
    loudness = 1.0
    for dim, parts in pieces:
        draws = jax.random.uniform(jax.random.fold_in(jax.random.fold_in(key, 6), dim), (parts,), jnp.float32, least / len(pieces), largest / len(pieces))
        loudness = loudness * jnp.repeat(jnp.exp(draws), extent[dim] // parts).reshape((-1,) + (1,) * (len(extent) - 1 - dim))
    return loudness


def setup_inputs(seed: int = 0) -> dict:
    keys = jax.random.split(jax.random.key(seed), 18)
    right_sides = draw_right_sides(jax.random.fold_in(keys[17], 71), 0)
    weights_fine = jnp.clip(2.0 * jax.random.uniform(keys[1], (NB0 * DEVICES, K, BS, BS), jnp.float32) ** block_levels(keys[1], (NB0 * DEVICES, K, BS, BS), ((0, 32),), -0.2, 0.2), 0.0, 2.0).astype(jnp.bfloat16)
    columns_fine = draw_columns_fine(jax.random.fold_in(keys[17], 71), 0)
    degree_fine = jnp.clip(jnp.exp(math.log(0.5) - 2.3025851 * jax.random.uniform(keys[3], (NB0 * DEVICES, BS), jnp.float32) ** block_levels(keys[3], (NB0 * DEVICES, BS), ((0, 32),), -0.2, 0.2)), 0.05, 0.5)
    owners_fine = draw_owners_fine(jax.random.fold_in(keys[17], 71), 0)
    slots_fine = place_ends(jax.random.randint(keys[5], (NB0 * DEVICES, BS), 0, NB1 * BS), jax.random.fold_in(keys[5], 1), 0, (NB1 * BS) - 1).astype(jnp.int32)
    weights_second = jnp.clip(8.0 * jax.random.uniform(keys[6], (NB1 * DEVICES, K, BS, BS), jnp.float32) ** block_levels(keys[6], (NB1 * DEVICES, K, BS, BS), ((0, 32),), -0.2, 0.2), 0.0, 8.0).astype(jnp.bfloat16)
    columns_second = draw_columns_second(jax.random.fold_in(keys[17], 71), 0)
    degree_second = jnp.clip(jnp.exp(math.log(2.0) - 2.3025851 * jax.random.uniform(keys[8], (NB1 * DEVICES, BS), jnp.float32) ** block_levels(keys[8], (NB1 * DEVICES, BS), ((0, 32),), -0.2, 0.2)), 0.2, 2.0)
    owners_second = draw_owners_second(jax.random.fold_in(keys[17], 71), 0)
    slots_second = place_ends(jax.random.randint(keys[10], (NB1 * DEVICES, BS), 0, NB2 * BS), jax.random.fold_in(keys[10], 1), 0, (NB2 * BS) - 1).astype(jnp.int32)
    weights_third = jnp.clip(32.0 * jax.random.uniform(keys[11], (NB2 * DEVICES, K, BS, BS), jnp.float32) ** block_levels(keys[11], (NB2 * DEVICES, K, BS, BS), ((0, 32),), -0.2, 0.2), 0.0, 32.0).astype(jnp.bfloat16)
    columns_third = draw_columns_third(jax.random.fold_in(keys[17], 71), 0)
    degree_third = jnp.clip(jnp.exp(math.log(8.0) - 2.3025851 * jax.random.uniform(keys[13], (NB2 * DEVICES, BS), jnp.float32) ** block_levels(keys[13], (NB2 * DEVICES, BS), ((0, 32),), -0.2, 0.2)), 0.8, 8.0)
    owners_third = draw_owners_third(jax.random.fold_in(keys[17], 71), 0)
    slots_third = place_ends(jax.random.randint(keys[15], (NB2 * DEVICES, BS), 0, C3), jax.random.fold_in(keys[15], 1), 0, C3 - 1).astype(jnp.int32)
    coarse_inverse = draw_coarse_inverse(jax.random.fold_in(keys[17], 71), 0)
    return dict(right_sides=right_sides, weights_fine=weights_fine, columns_fine=columns_fine, degree_fine=degree_fine, owners_fine=owners_fine, slots_fine=slots_fine, weights_second=weights_second, columns_second=columns_second, degree_second=degree_second, owners_second=owners_second, slots_second=slots_second, weights_third=weights_third, columns_third=columns_third, degree_third=degree_third, owners_third=owners_third, slots_third=slots_third, coarse_inverse=coarse_inverse)


damping = 0.8


def gather_rows(blocks):
    return jnp.transpose(blocks, (0, 2, 1)).reshape(-1, RHS_COUNT)


def make_blocks(rows_data):
    return jnp.transpose(rows_data.reshape(-1, BS, RHS_COUNT), (0, 2, 1))


def complete_diagonal_entries(weights, shift):
    return shift + jnp.sum(weights, axis=(1, 2), dtype=jnp.float32) / (K * BS)


def apply_operator(current_iterate, weights, columns, degree):
    total = current_iterate.shape[0]
    per_device = total // DEVICES
    rounded = lax.optimization_barrier(current_iterate.astype(jnp.bfloat16))
    widened = rounded.astype(jnp.float32)
    shaped_weights = weights.reshape(DEVICES, per_device, K, BS, BS)
    shaped_columns = columns.reshape(DEVICES, per_device, K)

    def per_block(packed):
        block_weights, block_columns = packed
        picked = widened[block_columns]
        return jnp.einsum("nkrb,nkbc->nrc", picked, block_weights.astype(jnp.float32), precision=lax.Precision.HIGHEST)

    product = lax.map(per_block, (shaped_weights, shaped_columns)).reshape(total, RHS_COUNT, BS)
    return degree[:, None, :] * current_iterate - product / (K * BS)


def reference(right_sides, weights_fine, columns_fine, degree_fine, owners_fine, slots_fine, weights_second, columns_second, degree_second, owners_second, slots_second, weights_third, columns_third, degree_third, owners_third, slots_third, coarse_inverse):
    levels = [(weights_fine, columns_fine, complete_diagonal_entries(weights_fine, degree_fine), owners_fine, slots_fine, NB1 * BS),
              (weights_second, columns_second, complete_diagonal_entries(weights_second, degree_second), owners_second, slots_second, NB2 * BS),
              (weights_third, columns_third, complete_diagonal_entries(weights_third, degree_third), owners_third, slots_third, C3)]
    source = right_sides.astype(jnp.float32)
    stored = []
    coarse_rows = None
    for position in range(3):
        weights, columns, degree, aggregate_owners, slots, coarse_count = levels[position]
        scale = degree[:, None, :]
        current_iterate = damping * source / scale
        for repeat in range(SWEEPS - 1):
            current_iterate = current_iterate + damping * (source - apply_operator(current_iterate, weights, columns, degree)) / scale
        residual = source - apply_operator(current_iterate, weights, columns, degree)
        stored.append((current_iterate, source))
        targets = (aggregate_owners * coarse_count + slots).reshape(-1).astype(jnp.int32)
        coarse_rows = jax.ops.segment_sum(gather_rows(residual), targets, num_segments=DEVICES * coarse_count)
        if position < 2:
            source = make_blocks(coarse_rows)
    aggregated_values = lax.optimization_barrier(coarse_rows.astype(jnp.bfloat16)).astype(jnp.float32).reshape(N_ROW, M3, RHS_COUNT)
    inverse_matrix = coarse_inverse.astype(jnp.float32).reshape(N_ROW, M3, M3)
    coarse_correction_rows = jnp.einsum("dut,dtx->dux", inverse_matrix, aggregated_values, precision=lax.Precision.HIGHEST).reshape(-1, RHS_COUNT)
    current_iterate = None
    for position in (2, 1, 0):
        weights, columns, degree, aggregate_owners, slots, coarse_count = levels[position]
        current_iterate, source = stored[position]
        targets = (aggregate_owners * coarse_count + slots).reshape(-1).astype(jnp.int32)
        current_iterate = current_iterate + make_blocks(coarse_correction_rows[targets])
        scale = degree[:, None, :]
        for repeat in range(SWEEPS):
            current_iterate = current_iterate + damping * (source - apply_operator(current_iterate, weights, columns, degree)) / scale
        coarse_correction_rows = gather_rows(current_iterate)
    return current_iterate
```

```python
import functools

import jax
import jax.numpy as jnp
from jax import lax
from jax.experimental import pallas as pl
from jax.experimental.pallas import tpu as pltpu
from jax.sharding import PartitionSpec as P

F32 = jnp.float32
BF16 = jnp.bfloat16
MESH = pl.DeviceIdType.MESH
DAMPING = 0.8
SPLIT_OWN = False


def loop(low, high, body, unroll=4):
    count = high - low
    if count <= 0:
        return
    while count % unroll:
        unroll -= 1

    if count == unroll:
        for inner in range(count):
            body(low + inner)
        return

    def step(outer, carry):
        for inner in range(unroll):
            body(low + outer * unroll + inner)
        return carry

    lax.fori_loop(0, count // unroll, step, 0)


def grouped(low, high, first, then, unroll=7):
    count = high - low
    if count <= 0:
        return
    while count % unroll:
        unroll -= 1

    def group(start):
        made = [first(start + inner) for inner in range(unroll)]
        for inner in range(unroll):
            then(start + inner, made[inner])

    if count == unroll:
        group(low)
        return

    def step(outer, carry):
        group(low + outer * unroll)
        return carry

    lax.fori_loop(0, count // unroll, step, 0)


class Level:
    def __init__(self, blocks, coarse, rhs_count, bs, k, ref, hbm, columns, ops):
        self.n, self.t, self.r, self.bs, self.k = blocks, coarse, rhs_count, bs, k
        self.ref, self.hbm, self.columns, self.ops = ref, hbm, columns, ops
        self.single = blocks < 4
        self.base = ops.me * blocks
        self.scale = 1.0 / (k * bs)

    def edges(self):
        n = self.n
        if self.single:
            return list(range(n))
        return [0, 1, n - 2, n - 1]

    def inner(self):
        return (0, 0) if self.single else (2, self.n - 2)

    def column(self, b, k):
        return self.columns[b, k] if self.single else self.columns[k, b]

    def weight_sums(self, b):
        w = self.ref["w"][b]
        return jnp.dot(jnp.ones((8, w.shape[0]), BF16), w, preferred_element_type=F32)

    def put_diagonal(self, b, total):
        degree = self.ref["deg"][pl.ds(b, 1), :]
        g = degree + total * self.scale
        self.ref["g"][b] = g
        self.ref["gi"][b] = DAMPING / g

    def row(self, name, b):
        value = self.ref[name][b, 0:1, :]
        return jnp.broadcast_to(value, (self.r, self.bs))

    def f(self, b):
        return self.ref["f"][b].astype(F32)

    def product(self, i, b, where):
        if where == "inner":
            buf, offset = self.ref[f"vb{i}"], self.base
        elif where == "low":
            buf, offset = self.ref[f"lo{i}"], self.base - 2
        else:
            buf, offset = self.ref[f"hi{i}"], self.base + self.n - 4
        top = buf.shape[0] - 1
        picked = [
            buf[jnp.clip(self.column(b, k) - offset, 0, top)] for k in range(self.k)
        ]
        left = jnp.concatenate(picked, axis=1)
        return jnp.dot(left, self.ref["w"][b], preferred_element_type=F32) * self.scale

    def halo_copies(self, i):
        n, ops, vb = self.n, self.ops, self.ref[f"vb{i}"]
        if self.single:
            low_dst, high_dst = self.ref[f"lo{i}"].at[0:2], self.ref[f"lo{i}"].at[4:6]
        else:
            low_dst, high_dst = self.ref[f"lo{i}"].at[0:2], self.ref[f"hi{i}"].at[4:6]
        return ops.pair(vb.at[n - 2 : n], low_dst, vb.at[0:2], high_dst, self.ref["sem"] + i)

    def fill_edges(self, i):
        n = self.n
        if self.single:
            self.ref[f"lo{i}"][2:4] = self.ref[f"vb{i}"][0:2]
        else:
            self.ref[f"lo{i}"][2:6] = self.ref[f"vb{i}"][0:4]
            self.ref[f"hi{i}"][0:4] = self.ref[f"vb{i}"][n - 4 : n]

    def run_edges(self, i, body):
        made = [self.product(i, b, "low" if b < 2 else "high") for b in self.edges()]
        for b, product in zip(self.edges(), made):
            body(b, product)

    def apply(self, i, body):
        grouped(*self.inner(), lambda b: self.product(i, b, "inner"), body)
        self.fill_edges(i)
        self.ops.wait(self.halo_copies(i))
        self.run_edges(i, body)

    def start_block(self, b):
        self.ref["vb0"][b] = (self.row("gi", b) * self.f(b)).astype(BF16)

    def first_sweep(self, b, product):
        f, gi = self.f(b), self.row("gi", b)
        x0 = gi * f
        x = (1.0 - DAMPING) * x0 + gi * (f + product)
        self.ref["x"][b] = x
        self.ref["vb1"][b] = x.astype(BF16)

    def residual(self, b, product):
        res = self.f(b) - self.row("g", b) * self.ref["x"][b] + product
        rel = self.owner(b)
        columns = pl.ds(pl.multiple_of(b * self.bs, self.bs), self.bs)
        rows = self.r
        high = res.astype(BF16)
        zero = jnp.zeros_like(res)
        out = self.ref["res"]
        out[0:rows, columns] = jnp.where(rel < 0, res, zero).astype(BF16)
        out[rows : 2 * rows, columns] = jnp.where(rel > 0, res, zero).astype(BF16)
        own = jnp.where(rel == 0, res, zero)
        high = own.astype(BF16)
        out[2 * rows : 3 * rows, columns] = high
        if SPLIT_OWN:
            out[3 * rows : 4 * rows, columns] = (own - high.astype(F32)).astype(BF16)

    def owner(self, b):
        value = self.ref["own"][pl.ds(b, 1), :] - self.ops.me
        return jnp.broadcast_to(value, (self.r, self.bs))

    def make_onehot(self, b):
        columns = pl.ds(pl.multiple_of(b * self.bs, self.bs), self.bs)
        slots = jnp.broadcast_to(self.ref["slot"][pl.ds(b, 1), :], (self.t, self.bs))
        index = lax.broadcasted_iota(jnp.int32, (self.t, self.bs), 0)
        self.ref["oh"][:, columns] = jnp.where(index == slots, 1.0, 0.0).astype(BF16)

    def restricted(self, rows, put):
        tile = min(self.t, 256)

        def body(j):
            at = pl.ds(pl.multiple_of(j * tile, tile), tile)
            put(
                at,
                lax.dot_general(
                    self.ref["res"][rows, :],
                    self.ref["oh"][at, :],
                    (((1,), (1,)), ((), ())),
                    preferred_element_type=F32,
                ),
            )

        loop(0, self.t // tile, body, 1)

    def restrict_copies(self):
        out, got = self.ref["rout"], self.ref["rin"]
        return self.ops.pair(out.at[1], got.at[0], out.at[0], got.at[1], self.ref["sem"] + 4)

    def restrict(self, into):
        r = self.r

        def put_out(at, value):
            self.ref["rout"][0, :, at] = value[0:r].astype(BF16)
            self.ref["rout"][1, :, at] = value[r : 2 * r].astype(BF16)

        self.restricted(slice(0, 2 * r), put_out)
        copies = self.restrict_copies()
        self.ops.start(copies)

        def put_own(at, value):
            if SPLIT_OWN:
                value = value[0:r] + value[r : 2 * r]
            self.ref["rown"][:, at] = value

        self.restricted(slice(2 * r, (4 if SPLIT_OWN else 3) * r), put_own)
        self.ops.wait(copies)
        for block in range(self.t // self.bs):
            at = slice(block * self.bs, (block + 1) * self.bs)
            into(
                block,
                self.ref["rown"][:, at]
                + self.ref["rin"][0, :, at].astype(F32)
                + self.ref["rin"][1, :, at].astype(F32),
            )

    def down(self, into, while_first=None, while_second=None):
        self.ops.start(self.halo_copies(0))
        loop(*self.inner(), self.start_block)
        if while_first is not None:
            while_first()
        self.apply(0, self.first_sweep)
        self.ops.start(self.halo_copies(1))
        if while_second is not None:
            while_second()
        self.apply(1, self.residual)
        self.restrict(into)

    def prolong_copies(self):
        out, got = self.ref["uout"], self.ref["uin"]
        return self.ops.pair(out, got.at[0], out, got.at[1], self.ref["sem"] + 5)

    def pair_columns(self, pair):
        return pl.ds(pl.multiple_of(pair * 2 * self.bs, 2 * self.bs), 2 * self.bs)

    def own_part(self, pair):
        return jnp.dot(
            self.ref["uout"][...], self.ref["oh"][:, self.pair_columns(pair)],
            preferred_element_type=F32,
        )

    def add_own(self, pair, value):
        for half in range(2):
            b = 2 * pair + half
            part = value[:, half * self.bs : (half + 1) * self.bs]
            self.ref["x"][b] = self.ref["x"][b] + jnp.where(self.owner(b) == 0, part, 0.0)

    def others_part(self, pair):
        left = jnp.concatenate([self.ref["uin"][0], self.ref["uin"][1]], axis=0)
        return jnp.dot(
            left, self.ref["oh"][:, self.pair_columns(pair)], preferred_element_type=F32
        )

    def add_others(self, pair, value):
        for half in range(2):
            b = 2 * pair + half
            at = slice(half * self.bs, (half + 1) * self.bs)
            rel = self.owner(b)
            x = self.ref["x"][b]
            x = x + jnp.where(rel < 0, value[0 : self.r, at], 0.0)
            x = x + jnp.where(rel > 0, value[self.r : 2 * self.r, at], 0.0)
            self.ref["x"][b] = x
            self.ref["vb2"][b] = x.astype(BF16)

    def sweep(self, i, last, out=None):
        def body(b, product):
            gi = self.row("gi", b)
            x = (1.0 - DAMPING) * self.ref["x"][b] + gi * (self.f(b) + product)
            self.ref["x"][b] = x
            if not last:
                self.ref[f"vb{i + 1}"][b] = x.astype(BF16)
            elif out is not None:
                out(b, x)

        return body

    def up(self, out=None):
        copies = self.prolong_copies()
        self.ops.start(copies)
        pairs = self.n // 2
        grouped(0, pairs, self.own_part, self.add_own, 2)
        self.ops.wait(copies)
        ends = [0] if self.single else [0, pairs - 1]
        made = [self.others_part(pair) for pair in ends]
        for pair, value in zip(ends, made):
            self.add_others(pair, value)
        self.ops.start(self.halo_copies(2))
        if not self.single:
            grouped(1, pairs - 1, self.others_part, self.add_others, 2)
        self.apply(2, self.sweep(2, False))
        self.ops.start(self.halo_copies(3))
        self.apply(3, self.sweep(3, True, out))

    def drain(self):
        for i in range(4):
            self.ops.drain(self.halo_copies(i))
        self.ops.drain(self.restrict_copies())
        self.ops.drain(self.prolong_copies())

    def clear_ends(self):
        for name, first, last in (("rin", 0, 1), ("uin", 0, 1)):
            ref = self.ref[name]

            @pl.when(self.ops.me == 0)
            def _():
                ref[first] = jnp.zeros(ref.shape[1:], ref.dtype)

            @pl.when(self.ops.me == self.ops.total - 1)
            def _():
                ref[last] = jnp.zeros(ref.shape[1:], ref.dtype)


class Ops:
    def __init__(self, send, recv):
        self.send, self.recv = send, recv
        self.rows, self.cols = lax.axis_size("row"), lax.axis_size("col")
        self.total = self.rows * self.cols
        self.row, self.col = lax.axis_index("row"), lax.axis_index("col")
        self.me = self.row * self.cols + self.col
        right = jnp.minimum(self.me + 1, self.total - 1)
        left = jnp.maximum(self.me - 1, 0)
        self.right = (right // self.cols, right % self.cols)
        self.left = (left // self.cols, left % self.cols)
        self.has_right = self.me < self.total - 1
        self.has_left = self.me > 0

    def pair(self, to_right, at_right, to_left, at_left, slot):
        first = pltpu.make_async_remote_copy(
            to_right, at_right, self.send.at[slot, 0], self.recv.at[slot, 0],
            device_id=self.right, device_id_type=MESH,
        )
        second = pltpu.make_async_remote_copy(
            to_left, at_left, self.send.at[slot, 1], self.recv.at[slot, 1],
            device_id=self.left, device_id_type=MESH,
        )
        return first, second

    def start(self, copies):
        pl.when(self.has_right)(lambda: copies[0].start())
        pl.when(self.has_left)(lambda: copies[1].start())

    def wait(self, copies):
        pl.when(self.has_left)(lambda: copies[0].wait_recv())
        pl.when(self.has_right)(lambda: copies[1].wait_recv())

    def drain(self, copies):
        pl.when(self.has_right)(lambda: copies[0].wait_send())
        pl.when(self.has_left)(lambda: copies[1].wait_send())


LEVEL_HBM = ("w", "deg", "own", "slot")
LEVEL_SCRATCH = (
    "w", "deg", "own", "slot", "g", "gi", "x", "vb0", "vb1", "vb2", "vb3",
    "lo0", "lo1", "lo2", "lo3", "hi0", "hi1", "hi2", "hi3", "res", "oh",
    "rout", "rin", "rown", "uout", "uin",
)


def kernel(sizes, rhs_count, bs, k, coarse_all, *refs):
    refs = list(refs)
    take = lambda count: [refs.pop(0) for _ in range(count)]
    rhs_hbm, inverse_hbm = take(2)
    columns_hbm, hbm = [], []
    for _ in sizes:
        columns_hbm.append(refs.pop(0))
        hbm.append(dict(zip(LEVEL_HBM, take(4))))
    (out,) = take(1)
    scratch = [dict(zip(LEVEL_SCRATCH, take(len(LEVEL_SCRATCH)))) for _ in sizes]
    columns = take(len(sizes))
    rhs, f_second, f_third, inverse, gathered = take(5)
    send, recv, gather_send, gather_recv, local = take(5)

    ops = Ops(send, recv)
    levels = []
    for position, (n, t) in enumerate(sizes):
        ref = scratch[position]
        ref["sem"] = position * 6
        ref["f"] = (rhs, f_second, f_third)[position]
        levels.append(Level(n, t, rhs_count, bs, k, ref, hbm[position], columns[position], ops))
    fine, second, third = levels

    loads = []

    def load(src, dst):
        copy = pltpu.make_async_copy(src, dst, local.at[len(loads)])
        loads.append(copy)
        copy.start()
        return copy

    n = fine.n
    early = []
    for at in (slice(0, 2), slice(n - 2, n)):
        early.append(load(hbm[0]["w"].at[at], scratch[0]["w"].at[at]))
    early.append(load(hbm[0]["deg"], scratch[0]["deg"]))
    early.append(load(rhs_hbm, rhs))
    for src, dst in zip(columns_hbm, columns):
        early.append(load(src, dst))
    middle = load(hbm[0]["w"].at[2 : n - 2], scratch[0]["w"].at[2 : n - 2])
    later = [
        load(hbm[0][name], scratch[0][name]) for name in ("own", "slot")
    ]
    for position in (1, 2):
        later += [load(hbm[position][name], scratch[position][name]) for name in LEVEL_HBM]
    later.append(load(inverse_hbm, inverse))

    barrier = pltpu.get_barrier_semaphore()
    next_row = jnp.logical_and(ops.has_right, ops.col == ops.cols - 1)
    previous_row = jnp.logical_and(ops.has_left, ops.col == 0)
    pl.when(next_row)(
        lambda: pl.semaphore_signal(barrier, inc=1, device_id=ops.right, device_id_type=MESH)
    )
    pl.when(previous_row)(
        lambda: pl.semaphore_signal(barrier, inc=1, device_id=ops.left, device_id_type=MESH)
    )
    for step in range(1, ops.cols):
        peer = lax.rem(ops.col + step, ops.cols)
        pl.semaphore_signal(barrier, inc=1, device_id=(ops.row, peer), device_id_type=MESH)
    for level in levels:
        level.clear_ends()
    for copy in early:
        copy.wait()
    def diagonal_and_start(b, total):
        fine.put_diagonal(b, total)
        fine.start_block(b)

    made = [fine.weight_sums(b) for b in fine.edges()]
    for b, total in zip(fine.edges(), made):
        diagonal_and_start(b, total)
    middle.wait()
    grouped(*fine.inner(), fine.weight_sums, diagonal_and_start)
    pl.semaphore_wait(
        barrier, ops.cols - 1 + next_row.astype(jnp.int32) + previous_row.astype(jnp.int32)
    )
    fine.ops.start(fine.halo_copies(0))
    for copy in later:
        copy.wait()
    loop(0, fine.n // 2, fine.make_onehot, 1)
    fine.apply(0, fine.first_sweep)
    fine.ops.start(fine.halo_copies(1))
    loop(fine.n // 2, fine.n, fine.make_onehot, 1)
    for level in (second, third):
        loop(0, level.n, level.make_onehot, 1)
        grouped(0, level.n, level.weight_sums, level.put_diagonal, 8)
    fine.apply(1, fine.residual)

    def into_level(level):
        def into(block, value):
            level.ref["f"][block] = value

        return into

    fine.restrict(into_level(second))
    for level, following in ((second, third), (third, None)):
        for b in level.edges():
            level.start_block(b)
        if following is not None:
            level.down(into_level(following))
        else:

            def into_coarse(block, value):
                gathered[ops.col] = value.astype(BF16)

            level.down(into_coarse)

    sends = []
    for step in range(1, ops.cols):
        peer = lax.rem(ops.col + step, ops.cols)
        copy = pltpu.make_async_remote_copy(
            gathered.at[ops.col], gathered.at[ops.col],
            gather_send.at[step - 1], gather_recv.at[step - 1],
            device_id=(ops.row, peer), device_id_type=MESH,
        )
        copy.start()
        sends.append(copy)
    for step in range(1, ops.cols):
        source = lax.rem(ops.col + ops.cols - step, ops.cols)
        pltpu.make_async_remote_copy(
            gathered.at[source], gathered.at[source],
            gather_send.at[step - 1], gather_recv.at[step - 1],
            device_id=(ops.row, source), device_id_type=MESH,
        ).wait_recv()
    everything = jnp.concatenate([gathered[p] for p in range(ops.cols)], axis=1)
    solved = lax.dot_general(
        everything, inverse[...], (((1,), (1,)), ((), ())), preferred_element_type=F32
    )
    third.ref["uout"][...] = solved.astype(BF16)

    def into_coarse_vector(level):
        def put(b, x):
            level.ref["uout"][:, b * bs : (b + 1) * bs] = x.astype(BF16)

        return put

    third.up(into_coarse_vector(second))
    second.up(into_coarse_vector(fine))

    def put_out(b, x):
        out[b] = x

    fine.up(put_out)
    for level in levels:
        level.drain()
    for copy in sends:
        copy.wait_send()


def on_device(
    right_sides,
    weights_fine, columns_fine, degree_fine, owners_fine, slots_fine,
    weights_second, columns_second, degree_second, owners_second, slots_second,
    weights_third, columns_third, degree_third, owners_third, slots_third,
    coarse_inverse,
):
    n0, r, bs = right_sides.shape
    n1, n2 = weights_second.shape[0], weights_third.shape[0]
    k = weights_fine.shape[1]
    c3, m3 = coarse_inverse.shape
    cols = lax.axis_size("col")
    sizes = ((n0, n1 * bs), (n1, n2 * bs), (n2, c3))
    merged = lambda w: w.reshape(w.shape[0], k * bs, bs)
    args = [right_sides, coarse_inverse]
    specs = [pl.BlockSpec(memory_space=pltpu.HBM)] * 2
    for w, c, d, o, s in (
        (weights_fine, columns_fine, degree_fine, owners_fine, slots_fine),
        (weights_second, columns_second, degree_second, owners_second, slots_second),
        (weights_third, columns_third, degree_third, owners_third, slots_third),
    ):
        args += [c.T if c.shape[0] >= 4 else c, merged(w), d, o, s]
        specs += [pl.BlockSpec(memory_space=pltpu.HBM)] * 5
    scratch = []
    for n, t in sizes:
        scratch += [
            pltpu.VMEM((n, k * bs, bs), BF16),
            pltpu.VMEM((n, bs), F32),
            pltpu.VMEM((n, bs), jnp.int32),
            pltpu.VMEM((n, bs), jnp.int32),
            pltpu.VMEM((n, 8, bs), F32),
            pltpu.VMEM((n, 8, bs), F32),
            pltpu.VMEM((n, r, bs), F32),
            *[pltpu.VMEM((n, r, bs), BF16)] * 4,
            *[pltpu.VMEM((6, r, bs), BF16)] * 8,
            pltpu.VMEM(((4 if SPLIT_OWN else 3) * r, n * bs), BF16),
            pltpu.VMEM((t, n * bs), BF16),
            pltpu.VMEM((2, r, t), BF16),
            pltpu.VMEM((2, r, t), BF16),
            pltpu.VMEM((r, t), F32),
            pltpu.VMEM((r, t), BF16),
            pltpu.VMEM((2, r, t), BF16),
        ]
    scratch += [
        pltpu.SMEM((k, n0), jnp.int32),
        pltpu.SMEM((k, n1), jnp.int32),
        pltpu.SMEM((n2, k), jnp.int32),
        pltpu.VMEM((n0, r, bs), BF16),
        pltpu.VMEM((n1, r, bs), F32),
        pltpu.VMEM((n2, r, bs), F32),
        pltpu.VMEM((c3, m3), BF16),
        pltpu.VMEM((cols, r, c3), BF16),
        pltpu.SemaphoreType.DMA((18, 2)),
        pltpu.SemaphoreType.DMA((18, 2)),
        pltpu.SemaphoreType.DMA((cols,)),
        pltpu.SemaphoreType.DMA((cols,)),
        pltpu.SemaphoreType.DMA((24,)),
    ]
    return pl.pallas_call(
        functools.partial(kernel, sizes, r, bs, k, m3),
        out_shape=jax.ShapeDtypeStruct((n0, r, bs), F32),
        in_specs=specs,
        out_specs=pl.BlockSpec(memory_space=pltpu.VMEM),
        scratch_shapes=scratch,
        compiler_params=pltpu.CompilerParams(
            collective_id=0, has_side_effects=True, vmem_limit_bytes=48 * 1024 * 1024
        ),
        name="vcycle",
    )(*[pltpu.with_memory_space_constraint(a, pltpu.HBM) for a in args])


def solution(mesh):
    whole = ("row", "col")
    vector, matrix, table = P(whole, None, None), P(whole, None, None, None), P(whole, None)
    level = (matrix, table, table, table, table)
    return jax.shard_map(
        on_device,
        mesh=mesh,
        in_specs=(vector, *level, *level, *level, table),
        out_specs=vector,
        check_vma=False,
    )
```

```python
import functools

import jax
import jax.numpy as jnp
from jax import lax
from jax.experimental import pallas as pl
from jax.experimental.pallas import tpu as pltpu
from jax.sharding import PartitionSpec as P

F32 = jnp.float32
BF16 = jnp.bfloat16
MESH = pl.DeviceIdType.MESH
DAMPING = 0.8


def loop(low, high, body, unroll=4):
    count = high - low
    if count <= 0:
        return
    while count % unroll:
        unroll -= 1

    if count == unroll:
        for inner in range(count):
            body(low + inner)
        return

    def step(outer, carry):
        for inner in range(unroll):
            body(low + outer * unroll + inner)
        return carry

    lax.fori_loop(0, count // unroll, step, 0)


def grouped(low, high, first, then, unroll=7):
    count = high - low
    if count <= 0:
        return
    while count % unroll:
        unroll -= 1

    def group(start):
        made = [first(start + inner) for inner in range(unroll)]
        for inner in range(unroll):
            then(start + inner, made[inner])

    if count == unroll:
        group(low)
        return

    def step(outer, carry):
        group(low + outer * unroll)
        return carry

    lax.fori_loop(0, count // unroll, step, 0)


class Copy:
    def __init__(self, ops, descriptor, delta):
        self.ops, self.descriptor, self.delta = ops, descriptor, delta

    def start(self):
        pl.when(self.ops.has(self.delta))(lambda: self.descriptor.start())

    def wait(self):
        pl.when(self.ops.has(-self.delta))(lambda: self.descriptor.wait_recv())

    def drain(self):
        pl.when(self.ops.has(self.delta))(lambda: self.descriptor.wait_send())


def start(copies):
    for copy in copies:
        copy.start()


def wait(copies):
    for copy in copies:
        copy.wait()


class Ops:
    def __init__(self, send, recv):
        self.send, self.recv = send, recv
        self.rows, self.cols = lax.axis_size("row"), lax.axis_size("col")
        self.total = self.rows * self.cols
        self.row, self.col = lax.axis_index("row"), lax.axis_index("col")
        self.me = self.row * self.cols + self.col
        self.copies = []

    def has(self, delta):
        return self.me < self.total - delta if delta > 0 else self.me >= -delta

    def peer(self, delta):
        index = jnp.clip(self.me + delta, 0, self.total - 1)
        return (index // self.cols, index % self.cols)

    def across(self, delta):
        over = self.col + delta >= self.cols if delta > 0 else self.col + delta < 0
        return jnp.logical_and(self.has(delta), over)

    def copy(self, src, dst, delta):
        slot = len(self.copies)
        descriptor = pltpu.make_async_remote_copy(
            src, dst, self.send.at[slot], self.recv.at[slot],
            device_id=self.peer(delta), device_id_type=MESH,
        )
        self.copies.append(Copy(self, descriptor, delta))
        return self.copies[-1]


class Level:
    def __init__(self, n, t, r, bs, k, ref, columns, ops):
        self.n, self.t, self.r, self.bs, self.k = n, t, r, bs, k
        self.ref, self.columns, self.ops = ref, columns, ops
        self.base = ops.me * n
        self.scale = 1.0 / (k * bs)

    def weight_sums(self, b):
        w = self.ref["w"][b]
        return jnp.dot(jnp.ones((8, w.shape[0]), BF16), w, preferred_element_type=F32)

    def put_diagonal(self, b, total):
        degree = self.ref["deg"][pl.ds(b, 1), :]
        g = degree + total * self.scale
        self.ref["g"][b] = g
        self.ref["gi"][b] = DAMPING / g

    def spread(self, row):
        return jnp.broadcast_to(row, (self.r, self.bs))

    def hot(self, row):
        slots = jnp.broadcast_to(row, (self.t, self.bs))
        index = lax.broadcasted_iota(jnp.int32, (self.t, self.bs), 0)
        return jnp.where(index == slots, 1.0, 0.0).astype(BF16)

    def put_residual(self, columns, res, rel):
        rows = self.r
        out = self.ref["res"]
        zero = jnp.zeros_like(res)
        out[0:rows, columns] = jnp.where(rel < 0, res, zero).astype(BF16)
        out[rows : 2 * rows, columns] = jnp.where(rel == 0, res, zero).astype(BF16)
        out[2 * rows : 3 * rows, columns] = jnp.where(rel > 0, res, zero).astype(BF16)

    def restricted(self, res, hot):
        return lax.dot_general(
            res, hot, (((1,), (1,)), ((), ())), preferred_element_type=F32
        )


class Fine(Level):
    def __init__(self, *args):
        super().__init__(*args)
        ref, ops, n = self.ref, self.ops, self.n
        self.halo = []
        for i in range(4):
            vb = ref[f"vb{i}"]
            self.halo.append([
                ops.copy(vb.at[n - 2 : n], ref[f"lo{i}"].at[0:2], 1),
                ops.copy(vb.at[0:2], ref[f"hi{i}"].at[4:6], -1),
            ])
        self.prolong = [
            ops.copy(ref["uout"], ref["uin"].at[0], 1),
            ops.copy(ref["uout"], ref["uin"].at[1], -1),
        ]
        out, got = ref["rout"], ref["rin"]
        tiles = self.t // (2 * self.bs)
        last = tiles - 1
        self.tiles = [0, last] + list(range(1, last))
        self.restrict_copies = {}
        for j in self.tiles:
            at = slice(2 * j, 2 * j + 2)
            made = [
                ops.copy(out.at[2, at], got.at[0, at], 1),
                ops.copy(out.at[0, at], got.at[1, at], -1),
            ]
            if j == 0:
                made.append(ops.copy(out.at[1, at], ref["near"].at[1], -1))
                made.append(ops.copy(out.at[0, at], ref["far"].at[1], -2))
            if j == last:
                made.append(ops.copy(out.at[1, at], ref["near"].at[0], 1))
                made.append(ops.copy(out.at[2, at], ref["far"].at[0], 2))
            self.restrict_copies[j] = made

    def edges(self):
        return [0, 1, self.n - 2, self.n - 1]

    def inner(self):
        return 2, self.n - 2

    def row(self, name, b):
        return self.spread(self.ref[name][b, 0:1, :])

    def f(self, b):
        return self.ref["f"][b].astype(F32)

    def product(self, i, b, where):
        if where == "inner":
            buf, offset = self.ref[f"vb{i}"], self.base
        elif where == "low":
            buf, offset = self.ref[f"lo{i}"], self.base - 2
        else:
            buf, offset = self.ref[f"hi{i}"], self.base + self.n - 4
        top = buf.shape[0] - 1
        picked = [
            buf[jnp.clip(self.columns[k, b] - offset, 0, top)] for k in range(self.k)
        ]
        left = jnp.concatenate(picked, axis=1)
        return jnp.dot(left, self.ref["w"][b], preferred_element_type=F32) * self.scale

    def apply(self, i, body):
        grouped(*self.inner(), lambda b: self.product(i, b, "inner"), body)
        n = self.n
        self.ref[f"lo{i}"][2:6] = self.ref[f"vb{i}"][0:4]
        self.ref[f"hi{i}"][0:4] = self.ref[f"vb{i}"][n - 4 : n]
        wait(self.halo[i])
        made = [self.product(i, b, "low" if b < 2 else "high") for b in self.edges()]
        for b, product in zip(self.edges(), made):
            body(b, product)

    def start_block(self, b):
        self.ref["vb0"][b] = (self.row("gi", b) * self.f(b)).astype(BF16)

    def first_sweep(self, b, product):
        f, gi = self.f(b), self.row("gi", b)
        x0 = gi * f
        x = (1.0 - DAMPING) * x0 + gi * (f + product)
        self.ref["x"][b] = x
        self.ref["vb1"][b] = x.astype(BF16)

    def at(self, b):
        return pl.ds(pl.multiple_of(b * self.bs, self.bs), self.bs)

    def owner(self, b):
        return self.spread(self.ref["own"][pl.ds(b, 1), :] - self.ops.me)

    def residual(self, b, product):
        res = self.f(b) - self.row("g", b) * self.ref["x"][b] + product
        self.put_residual(self.at(b), res, self.owner(b))

    def make_onehot(self, b):
        self.ref["oh"][:, self.at(b)] = self.hot(self.ref["slot"][pl.ds(b, 1), :])

    def restrict(self):
        r, bs = self.r, self.bs
        for j in self.tiles:
            at = slice(2 * j * bs, (2 * j + 2) * bs)
            value = self.restricted(self.ref["res"][...], self.ref["oh"][at, :])
            for half in range(2):
                b = 2 * j + half
                part = value[:, half * bs : (half + 1) * bs]
                for way in range(3):
                    self.ref["rout"][way, b] = part[way * r : (way + 1) * r].astype(BF16)
                self.ref["rown"][b] = part[r : 2 * r]
            start(self.restrict_copies[j])

    def received(self, below):
        for j in self.tiles:
            wait(self.restrict_copies[j])
        got, out = self.ref["rin"], self.ref["rout"]
        n = below.n
        for b in range(n):
            below.ref["f"][b] = self.ref["rown"][b] + got[0, b].astype(F32) + got[1, b].astype(F32)
        for side, way, first in ((0, 0, n - 2), (1, 2, 0)):
            for j in range(2):
                below.ref["fn"][side, j] = (
                    self.ref["near"][side, j].astype(F32)
                    + self.ref["far"][side, j].astype(F32)
                    + out[way, first + j].astype(F32)
                )

    def pair_columns(self, pair):
        return pl.ds(pl.multiple_of(pair * 2 * self.bs, 2 * self.bs), 2 * self.bs)

    def own_part(self, pair):
        return jnp.dot(
            self.ref["uout"][...], self.ref["oh"][:, self.pair_columns(pair)],
            preferred_element_type=F32,
        )

    def add_own(self, pair, value):
        for half in range(2):
            b = 2 * pair + half
            part = value[:, half * self.bs : (half + 1) * self.bs]
            self.ref["x"][b] = self.ref["x"][b] + jnp.where(self.owner(b) == 0, part, 0.0)

    def others_part(self, pair):
        left = jnp.concatenate([self.ref["uin"][0], self.ref["uin"][1]], axis=0)
        return jnp.dot(
            left, self.ref["oh"][:, self.pair_columns(pair)], preferred_element_type=F32
        )

    def add_others(self, pair, value):
        for half in range(2):
            b = 2 * pair + half
            at = slice(half * self.bs, (half + 1) * self.bs)
            rel = self.owner(b)
            x = self.ref["x"][b]
            x = x + jnp.where(rel < 0, value[0 : self.r, at], 0.0)
            x = x + jnp.where(rel > 0, value[self.r : 2 * self.r, at], 0.0)
            self.ref["x"][b] = x
            self.ref["vb2"][b] = x.astype(BF16)

    def sweep(self, i, out):
        def body(b, product):
            x = (1.0 - DAMPING) * self.ref["x"][b] + self.row("gi", b) * (self.f(b) + product)
            if out is None:
                self.ref["x"][b] = x
                self.ref[f"vb{i + 1}"][b] = x.astype(BF16)
            else:
                out[b] = x

        return body

    def up(self, out):
        start(self.prolong)
        pairs = self.n // 2
        grouped(0, pairs, self.own_part, self.add_own, 2)
        wait(self.prolong)
        ends = [0, pairs - 1]
        made = [self.others_part(pair) for pair in ends]
        for pair, value in zip(ends, made):
            self.add_others(pair, value)
        start(self.halo[2])
        grouped(1, pairs - 1, self.others_part, self.add_others, 2)
        self.apply(2, self.sweep(2, None))
        start(self.halo[3])
        self.apply(3, self.sweep(3, out))

    def clear_ends(self):
        for name, low, high in (("rin", 0, 1), ("uin", 0, 1), ("near", 0, 1), ("far", 0, 1)):
            ref = self.ref[name]
            for entry, missing in ((low, -2 if name == "far" else -1), (high, 2 if name == "far" else 1)):

                @pl.when(jnp.logical_not(self.ops.has(missing)))
                def _():
                    ref[entry] = jnp.zeros(ref.shape[1:], ref.dtype)


class Small(Level):
    def __init__(self, n, t, r, bs, k, ref, columns, ops, halo, weight_ways, degree_ways, send_ways):
        super().__init__(n, t, r, bs, k, ref, columns[0], ops)
        self.halo, self.m = halo, min(n, 2)
        self.other_columns = columns[1:]
        self.weight_ways, self.degree_ways, self.send_ways = weight_ways, degree_ways, send_ways
        ways = weight_ways
        self.tables, self.weights = [], []
        for at, d in enumerate(ways):
            self.tables.append(ops.copy(ref["own"], ref["ownn"].at[at], -d))
            self.tables.append(ops.copy(ref["slot"], ref["slotn"].at[at], -d))
            self.tables.append(ops.copy(columns[0], columns[1 + at], -d))
        for at, d in enumerate(degree_ways):
            self.tables.append(ops.copy(ref["g"].at[self.edge(d)], ref["gn"].at[at], -d))
        for j in range(self.m):
            for rows in range(k):
                part = slice(rows * bs, (rows + 1) * bs)
                group = []
                for at, d in enumerate(ways):
                    source = self.edge(d).start + j
                    group.append(ops.copy(ref["w"].at[source, part], ref["wn"].at[at, j, part], -d))
                self.weights.append(group)
        self.sends = [
            ops.copy(ref["uout"], ref["uin"].at[at], -d) for at, d in enumerate(send_ways)
        ]

    def edge(self, d):
        return slice(self.n - self.m, self.n) if d < 0 else slice(0, self.m)

    def place(self, b):
        d = b // self.n
        j = b - d * self.n
        return d, j, j - self.edge(d).start

    def column(self, b, k):
        d, j, _ = self.place(b)
        table = self.columns if d == 0 else self.other_columns[self.weight_ways.index(d)]
        return table[j, k] if self.n < 4 else table[k, j]

    def w(self, b):
        d, j, e = self.place(b)
        return self.ref["w"][j] if d == 0 else self.ref["wn"][self.weight_ways.index(d), e]

    def row(self, name, b):
        d, j, e = self.place(b)
        if d == 0:
            return self.spread(self.ref[name][j, 0:1, :])
        return self.spread(self.ref[name + "n"][self.degree_ways.index(d), e, 0:1, :])

    def f(self, b):
        d, j, e = self.place(b)
        if d == 0:
            return self.ref["f"][j]
        return self.ref["fn"][self.degree_ways.index(d), e].astype(F32)

    def table(self, name, b):
        d, j, _ = self.place(b)
        if d == 0:
            return self.ref[name][j : j + 1, :]
        return self.ref[name + "n"][self.weight_ways.index(d), j : j + 1, :]

    def owner(self, b):
        return self.spread(self.table("own", b) - self.ops.me)

    def invert(self):
        for at in range(len(self.degree_ways)):
            for e in range(self.m):
                self.ref["gin"][at, e] = DAMPING / self.ref["gn"][at, e]

    def make_onehots(self, reach):
        for b in range(-reach, self.n + reach):
            at = (b + reach) * self.bs
            self.ref["oh"][:, at : at + self.bs] = self.hot(self.table("slot", b))

    def product(self, i, b):
        buf = self.ref[f"vb{i}"]
        offset = self.base - self.halo
        top = buf.shape[0] - 1
        picked = [
            buf[jnp.clip(self.column(b, k) - offset, 0, top)] for k in range(self.k)
        ]
        left = jnp.concatenate(picked, axis=1)
        return jnp.dot(left, self.w(b), preferred_element_type=F32) * self.scale

    def apply(self, i, blocks, body, size=6):
        blocks = list(blocks)
        for low in range(0, len(blocks), size):
            group = blocks[low : low + size]
            made = [self.product(i, b) for b in group]
            for b, product in zip(group, made):
                body(b, product)

    def start_blocks(self, low, high):
        for b in range(low, high):
            self.ref["vb0"][b + self.halo] = (self.row("gi", b) * self.f(b)).astype(BF16)

    def first_sweep(self, b, product):
        f, gi = self.f(b), self.row("gi", b)
        x0 = gi * f
        x = (1.0 - DAMPING) * x0 + gi * (f + product)
        self.ref["x"][b + self.halo] = x
        self.ref["vb1"][b + self.halo] = x.astype(BF16)

    def residual_of(self, b, product):
        return self.f(b) - self.row("g", b) * self.ref["x"][b + self.halo] + product

    def add_correction(self, reach):
        bs, r = self.bs, self.r
        corrections = {0: self.ref["uout"]}
        for at, d in enumerate(self.send_ways):
            corrections[d] = self.ref["uin"].at[at]
        for b in range(-reach, self.n + reach, 2):
            d, _, _ = self.place(b)
            left = jnp.concatenate([corrections[d + way][...] for way in (-1, 0, 1)], axis=0)
            at = (b + reach) * bs
            value = jnp.dot(left, self.ref["oh"][:, at : at + 2 * bs], preferred_element_type=F32)
            for half in range(2):
                part = value[:, half * bs : (half + 1) * bs]
                rel = self.owner(b + half) - d
                low, own, high = (part[way * r : (way + 1) * r] for way in range(3))
                add = jnp.where(rel == 0, own, jnp.where(rel < 0, low, high))
                x = self.ref["x"][b + half + self.halo] + add
                self.ref["x"][b + half + self.halo] = x
                self.ref["vb2"][b + half + self.halo] = x.astype(BF16)

    def sweep(self, i, out=None):
        def body(b, product):
            h = self.halo
            x = (1.0 - DAMPING) * self.ref["x"][b + h] + self.row("gi", b) * (self.f(b) + product)
            if out is None:
                self.ref["x"][b + h] = x
                self.ref[f"vb{i + 1}"][b + h] = x.astype(BF16)
            else:
                out(b, x)

        return body

    def up(self, out):
        start(self.sends)
        return self.sends

    def clear_ends(self):
        for at, d in enumerate(self.weight_ways):

            @pl.when(jnp.logical_not(self.ops.has(d)))
            def _():
                self.ref["ownn"][at] = jnp.full(self.ref["ownn"].shape[1:], -8, jnp.int32)
                self.ref["slotn"][at] = jnp.zeros(self.ref["slotn"].shape[1:], jnp.int32)
                self.ref["wn"][at] = jnp.zeros(self.ref["wn"].shape[1:], BF16)
                columns = self.other_columns[at]
                for i in range(columns.shape[0]):
                    for j in range(columns.shape[1]):
                        columns[i, j] = 0

        for at, d in enumerate(self.degree_ways):

            @pl.when(jnp.logical_not(self.ops.has(d)))
            def _():
                self.ref["gn"][at] = jnp.ones(self.ref["gn"].shape[1:], F32)
                self.ref["fn"][at] = jnp.zeros(self.ref["fn"].shape[1:], self.ref["fn"].dtype)

        for at, d in enumerate(self.send_ways):

            @pl.when(jnp.logical_not(self.ops.has(d)))
            def _():
                self.ref["uin"][at] = jnp.zeros(self.ref["uin"].shape[1:], BF16)


class Second(Small):
    def __init__(self, *args):
        super().__init__(*args, 4, (-1, 1), (-1, 1), (-2, -1, 1, 2))
        ref, ops, n, h = self.ref, self.ops, self.n, self.halo
        vb, got = ref["vb1"], ref["vin"]
        own = lambda low, high: vb.at[h + low : h + high]
        self.halo_near = [
            ops.copy(own(n - 2, n), got.at[0, 2:4], 1), ops.copy(own(0, 2), got.at[1, 0:2], -1)
        ]
        self.halo_far = [
            ops.copy(own(n - 4, n - 2), got.at[0, 0:2], 1), ops.copy(own(2, 4), got.at[1, 2:4], -1)
        ]
        self.restrict_copies = [
            ops.copy(ref["rout"].at[1], ref["rin"].at[0], 1),
            ops.copy(ref["rout"].at[0], ref["rin"].at[1], -1),
        ]

    def residual(self, b, product):
        at = slice(b * self.bs, (b + 1) * self.bs)
        self.put_residual(at, self.residual_of(b, product), self.owner(b))

    def down(self, below, meanwhile):
        n, h, r, bs = self.n, self.halo, self.r, self.bs
        self.start_blocks(-2, n + 2)
        edges = [0, 1, n - 2, n - 1]
        self.apply(0, edges, self.first_sweep)
        start(self.halo_near)
        self.apply(0, range(2, n - 2), self.first_sweep)
        start(self.halo_far)
        meanwhile()
        self.apply(1, range(2, n - 2), self.residual)
        wait(self.halo_near)
        self.ref["vb1"][h - 2 : h] = self.ref["vin"][0, 2:4]
        self.ref["vb1"][h + n : h + n + 2] = self.ref["vin"][1, 0:2]
        self.apply(1, edges, self.residual)
        reach = 4
        own = slice(reach * bs, (reach + n) * bs)
        value = self.restricted(self.ref["res"][...], self.ref["oh"][:, own])
        for b in range(below.n):
            at = slice(b * bs, (b + 1) * bs)
            self.ref["rout"][0, b] = value[0:r, at].astype(BF16)
            self.ref["rout"][1, b] = value[2 * r : 3 * r, at].astype(BF16)
        start(self.restrict_copies)
        for b in range(below.n):
            self.ref["rown"][b] = value[r : 2 * r, b * bs : (b + 1) * bs]

    def received(self, below):
        wait(self.restrict_copies)
        got = self.ref["rin"]
        for b in range(below.n):
            f = self.ref["rown"][b] + got[0, b].astype(F32) + got[1, b].astype(F32)
            below.ref["f"][b] = f
            below.ref["fout"][b] = f.astype(BF16)

    def finish(self, out):
        n, h = self.n, self.halo
        wait(self.halo_far)
        for j in range(4):
            self.ref["x"][h - 4 + j] = self.ref["vin"][0, j].astype(F32)
            self.ref["x"][h + n + j] = self.ref["vin"][1, j].astype(F32)
        wait(self.sends)
        self.add_correction(4)
        for group in self.weights:
            wait(group)
        self.apply(2, range(-2, n + 2), self.sweep(2))
        self.apply(3, range(n), self.sweep(3, out))

    def clear_ends(self):
        super().clear_ends()
        for name in ("rin", "vin"):
            for at, d in ((0, -1), (1, 1)):

                @pl.when(jnp.logical_not(self.ops.has(d)))
                def _():
                    self.ref[name][at] = jnp.zeros(self.ref[name].shape[1:], BF16)


class Third(Small):
    def __init__(self, *args):
        super().__init__(*args, 6, (-2, -1, 1, 2), (-3, -2, -1, 1, 2, 3), (-3, -2, -1, 1, 2, 3))
        ref, ops = self.ref, self.ops
        self.sources = [
            ops.copy(ref["fout"], ref["fn"].at[at], -d) for at, d in enumerate(self.degree_ways)
        ]

    def down(self, into):
        n, bs = self.n, self.bs
        wait(self.sources)
        self.start_blocks(-6, n + 6)
        for group in self.weights:
            wait(group)
        self.apply(0, range(-4, n + 4), self.first_sweep)

        def residual(b, product):
            res = self.residual_of(b, product)
            at = (b + 2) * bs
            kept = jnp.where(self.owner(b) == 0, res, jnp.zeros_like(res))
            self.ref["res"][:, at : at + bs] = kept.astype(BF16)

        self.apply(1, range(-2, n + 2), residual)
        near = slice(2 * bs, (n + 6) * bs)
        into(self.restricted(self.ref["res"][...], self.ref["oh"][:, near]))

    def finish(self, out):
        n = self.n
        wait(self.sends)
        self.add_correction(4)
        self.apply(2, range(-2, n + 2), self.sweep(2))
        self.apply(3, range(n), self.sweep(3, out))


LEVEL_HBM = ("w", "deg", "own", "slot")
SHARED = ("w", "deg", "own", "slot", "g", "gi", "x", "vb0", "vb1", "vb2", "vb3", "res", "oh", "uout", "uin")
FINE = SHARED + (
    "lo0", "lo1", "lo2", "lo3", "hi0", "hi1", "hi2", "hi3", "rout", "rin", "rown", "near", "far",
)
SMALL = SHARED + ("f", "fn", "wn", "ownn", "slotn", "gn", "gin")
SECOND = SMALL + ("rout", "rin", "rown", "vin")
THIRD = SMALL + ("fout",)


def kernel(sizes, rhs_count, bs, k, *refs):
    refs = list(refs)
    take = lambda count: [refs.pop(0) for _ in range(count)]
    rhs_hbm, inverse_hbm = take(2)
    columns_hbm, hbm = [], []
    for _ in sizes:
        columns_hbm.append(refs.pop(0))
        hbm.append(dict(zip(LEVEL_HBM, take(4))))
    (out,) = take(1)
    scratch = [dict(zip(names, take(len(names)))) for names in (FINE, SECOND, THIRD)]
    columns = [take(1), take(3), take(5)]
    rhs, inverse, gathered = take(3)
    send, recv, gather_send, gather_recv, local = take(5)

    ops = Ops(send, recv)
    scratch[0]["f"] = rhs
    (n0, t0), (n1, t1), (n2, t2) = sizes
    fine = Fine(n0, t0, rhs_count, bs, k, scratch[0], columns[0][0], ops)
    second = Second(n1, t1, rhs_count, bs, k, scratch[1], columns[1], ops)
    third = Third(n2, t2, rhs_count, bs, k, scratch[2], columns[2], ops)
    levels = [fine, second, third]

    loads = []

    def load(src, dst):
        copy = pltpu.make_async_copy(src, dst, local.at[len(loads)])
        loads.append(copy)
        copy.start()
        return copy

    n = fine.n
    early = []
    for at in (slice(0, 2), slice(n - 2, n)):
        early.append(load(hbm[0]["w"].at[at], scratch[0]["w"].at[at]))
    early.append(load(hbm[0]["deg"], scratch[0]["deg"]))
    early.append(load(rhs_hbm, rhs))
    for level in range(3):
        early.append(load(columns_hbm[level], columns[level][0]))
    middle = load(hbm[0]["w"].at[2 : n - 2], scratch[0]["w"].at[2 : n - 2])
    later = [load(hbm[0][name], scratch[0][name]) for name in ("own", "slot")]
    for position in (1, 2):
        later += [load(hbm[position][name], scratch[position][name]) for name in LEVEL_HBM]
    last = load(inverse_hbm, inverse)

    barrier = pltpu.get_barrier_semaphore()
    expected = ops.cols - 1
    for delta in (-3, -2, -1, 1, 2, 3):
        outside = ops.across(delta)
        pl.when(outside)(
            lambda: pl.semaphore_signal(
                barrier, inc=1, device_id=ops.peer(delta), device_id_type=MESH
            )
        )
        expected = expected + outside.astype(jnp.int32)
    for step in range(1, ops.cols):
        peer = lax.rem(ops.col + step, ops.cols)
        pl.semaphore_signal(barrier, inc=1, device_id=(ops.row, peer), device_id_type=MESH)
    for level in levels:
        level.clear_ends()
    for copy in early:
        copy.wait()

    def diagonal_and_start(b, total):
        fine.put_diagonal(b, total)
        fine.start_block(b)

    made = [fine.weight_sums(b) for b in fine.edges()]
    for b, total in zip(fine.edges(), made):
        diagonal_and_start(b, total)
    middle.wait()
    grouped(*fine.inner(), fine.weight_sums, diagonal_and_start)
    for copy in later:
        copy.wait()
    for level in (second, third):
        grouped(0, level.n, level.weight_sums, level.put_diagonal, 8)
    pl.semaphore_wait(barrier, expected)

    start(fine.halo[0])
    start(second.tables)
    start(third.tables)
    third_weights = list(third.weights)
    for _ in range(2):
        start(third_weights.pop(0))
    loop(0, n // 2, fine.make_onehot, 1)
    fine.apply(0, fine.first_sweep)
    start(fine.halo[1])
    for _ in range(2):
        start(third_weights.pop(0))
    loop(n // 2, n, fine.make_onehot, 1)
    fine.apply(1, fine.residual)
    fine.restrict()
    for level in (second, third):
        wait(level.tables)
        level.invert()
        level.make_onehots(4)
    fine.received(second)

    def rest_of_weights():
        while third_weights:
            start(third_weights.pop(0))

    second.down(third, rest_of_weights)
    second_weights = list(second.weights)
    for _ in range(2):
        start(second_weights.pop(0))
    second.received(third)
    start(third.sources)
    for _ in range(2):
        start(second_weights.pop(0))

    def into_coarse(value):
        gathered[ops.col] = value.astype(BF16)

    third.down(into_coarse)

    sends = []
    for step in range(1, ops.cols):
        peer = lax.rem(ops.col + step, ops.cols)
        copy = pltpu.make_async_remote_copy(
            gathered.at[ops.col], gathered.at[ops.col],
            gather_send.at[step - 1], gather_recv.at[step - 1],
            device_id=(ops.row, peer), device_id_type=MESH,
        )
        copy.start()
        sends.append(copy)
    last.wait()
    for step in range(1, ops.cols):
        source = lax.rem(ops.col + ops.cols - step, ops.cols)
        pltpu.make_async_remote_copy(
            gathered.at[source], gathered.at[source],
            gather_send.at[step - 1], gather_recv.at[step - 1],
            device_id=(ops.row, source), device_id_type=MESH,
        ).wait_recv()
    everything = jnp.concatenate([gathered[p] for p in range(ops.cols)], axis=1)
    solved = lax.dot_general(
        everything, inverse[...], (((1,), (1,)), ((), ())), preferred_element_type=F32
    )
    third.ref["uout"][...] = solved.astype(BF16)
    start(third.sends)
    while second_weights:
        start(second_weights.pop(0))

    def into_coarse_vector(level):
        def put(b, x):
            level.ref["uout"][:, b * bs : (b + 1) * bs] = x.astype(BF16)

        return put

    third.finish(into_coarse_vector(second))
    start(second.sends)
    second.finish(into_coarse_vector(fine))
    fine.up(out)
    for copy in ops.copies:
        copy.drain()
    for copy in sends:
        copy.wait_send()


def on_device(
    right_sides,
    weights_fine, columns_fine, degree_fine, owners_fine, slots_fine,
    weights_second, columns_second, degree_second, owners_second, slots_second,
    weights_third, columns_third, degree_third, owners_third, slots_third,
    coarse_inverse,
):
    n0, r, bs = right_sides.shape
    n1, n2 = weights_second.shape[0], weights_third.shape[0]
    k = weights_fine.shape[1]
    c3, m3 = coarse_inverse.shape
    cols = lax.axis_size("col")
    sizes = ((n0, n1 * bs), (n1, n2 * bs), (n2, c3))
    merged = lambda w: w.reshape(w.shape[0], k * bs, bs)
    args = [right_sides, coarse_inverse]
    for w, c, d, o, s in (
        (weights_fine, columns_fine, degree_fine, owners_fine, slots_fine),
        (weights_second, columns_second, degree_second, owners_second, slots_second),
        (weights_third, columns_third, degree_third, owners_third, slots_third),
    ):
        args += [c.T if c.shape[0] >= 4 else c, merged(w), d, o, s]
    specs = [pl.BlockSpec(memory_space=pltpu.HBM)] * len(args)
    vmem = pltpu.VMEM
    vector = lambda *lead: vmem((*lead, r, bs), BF16)

    def shared(n, t, window, ways, res, hot):
        return [
            vmem((n, k * bs, bs), BF16),
            vmem((n, bs), F32),
            vmem((n, bs), jnp.int32),
            vmem((n, bs), jnp.int32),
            vmem((n, 8, bs), F32),
            vmem((n, 8, bs), F32),
            vmem((window, r, bs), F32),
            *[vector(window)] * 4,
            vmem((res[0] * r, res[1] * bs), BF16),
            vmem((t, hot * bs), BF16),
            vmem((r, t), BF16),
            vmem((ways, r, t), BF16),
        ]

    def small(n, weights, degrees, source):
        m = min(n, 2)
        return [
            vmem((n, r, bs), F32),
            vmem((degrees, m, r, bs), source),
            vmem((weights, m, k * bs, bs), BF16),
            vmem((weights, n, bs), jnp.int32),
            vmem((weights, n, bs), jnp.int32),
            vmem((degrees, m, 8, bs), F32),
            vmem((degrees, m, 8, bs), F32),
        ]

    scratch = shared(n0, n1 * bs, n0, 2, (3, n0), n0)
    scratch += [vector(6)] * 8
    scratch += [vector(3, n1), vector(2, n1), vmem((n1, r, bs), F32), vector(2, 2), vector(2, 2)]
    scratch += shared(n1, n2 * bs, n1 + 8, 4, (3, n1), n1 + 8)
    scratch += small(n1, 2, 2, F32)
    scratch += [vector(2, n2), vector(2, n2), vmem((n2, r, bs), F32), vector(2, 4)]
    scratch += shared(n2, c3, n2 + 12, 6, (1, n2 + 4), n2 + 8)
    scratch += small(n2, 4, 6, BF16)
    scratch += [vector(n2)]
    scratch += [pltpu.SMEM((k, n0), jnp.int32)]
    scratch += [pltpu.SMEM((k, n1), jnp.int32)] * 3
    scratch += [pltpu.SMEM((n2, k), jnp.int32)] * 5
    scratch += [
        vector(n0),
        vmem((c3, m3), BF16),
        vmem((cols, r, c3), BF16),
        pltpu.SemaphoreType.DMA((140,)),
        pltpu.SemaphoreType.DMA((140,)),
        pltpu.SemaphoreType.DMA((cols,)),
        pltpu.SemaphoreType.DMA((cols,)),
        pltpu.SemaphoreType.DMA((24,)),
    ]
    return pl.pallas_call(
        functools.partial(kernel, sizes, r, bs, k),
        out_shape=jax.ShapeDtypeStruct((n0, r, bs), F32),
        in_specs=specs,
        out_specs=pl.BlockSpec(memory_space=pltpu.VMEM),
        scratch_shapes=scratch,
        compiler_params=pltpu.CompilerParams(
            collective_id=0, has_side_effects=True, vmem_limit_bytes=48 * 1024 * 1024
        ),
        name="vcycle",
    )(*[pltpu.with_memory_space_constraint(a, pltpu.HBM) for a in args])


def solution(mesh):
    whole = ("row", "col")
    vector, matrix, table = P(whole, None, None), P(whole, None, None, None), P(whole, None)
    level = (matrix, table, table, table, table)
    return jax.shard_map(
        on_device,
        mesh=mesh,
        in_specs=(vector, *level, *level, *level, table),
        out_specs=vector,
        check_vma=False,
    )
```

```python
import functools

import jax
import jax.numpy as jnp
from jax import lax
from jax.experimental import pallas as pl
from jax.experimental.pallas import tpu as pltpu
from jax.sharding import PartitionSpec as P

F32 = jnp.float32
BF16 = jnp.bfloat16
F8 = jnp.float8_e4m3fn
MESH = pl.DeviceIdType.MESH
DAMPING = 0.8
THIRD_SLOTS = (2, 1, 2, 1)
SECOND_SLOTS = (1, 1, 2, 2)


def loop(low, high, body, unroll=4):
    count = high - low
    if count <= 0:
        return
    while count % unroll:
        unroll -= 1

    if count == unroll:
        for inner in range(count):
            body(low + inner)
        return

    def step(outer, carry):
        for inner in range(unroll):
            body(low + outer * unroll + inner)
        return carry

    lax.fori_loop(0, count // unroll, step, 0)


def grouped(low, high, first, then, unroll=7):
    count = high - low
    if count <= 0:
        return
    while count % unroll:
        unroll -= 1

    def group(start):
        made = [first(start + inner) for inner in range(unroll)]
        for inner in range(unroll):
            then(start + inner, made[inner])

    if count == unroll:
        group(low)
        return

    def step(outer, carry):
        group(low + outer * unroll)
        return carry

    lax.fori_loop(0, count // unroll, step, 0)


class Copy:
    def __init__(self, ops, descriptor, delta):
        self.ops, self.descriptor, self.delta = ops, descriptor, delta

    def start(self):
        pl.when(self.ops.has(self.delta))(lambda: self.descriptor.start())

    def wait(self):
        pl.when(self.ops.has(-self.delta))(lambda: self.descriptor.wait_recv())

    def drain(self):
        pl.when(self.ops.has(self.delta))(lambda: self.descriptor.wait_send())


class Slots:
    def __init__(self, groups, counts):
        self.groups, self.counts = list(groups), list(counts)

    def send(self):
        for _ in range(self.counts.pop(0)):
            start(self.groups.pop(0))


def start(copies):
    for copy in copies:
        copy.start()


def wait(copies):
    for copy in copies:
        copy.wait()


class Ops:
    def __init__(self, send, recv):
        self.send, self.recv = send, recv
        self.rows, self.cols = lax.axis_size("row"), lax.axis_size("col")
        self.total = self.rows * self.cols
        self.row, self.col = lax.axis_index("row"), lax.axis_index("col")
        self.me = self.row * self.cols + self.col
        self.copies = []

    def has(self, delta):
        return self.me < self.total - delta if delta > 0 else self.me >= -delta

    def peer(self, delta):
        index = jnp.clip(self.me + delta, 0, self.total - 1)
        return (index // self.cols, index % self.cols)

    def across(self, delta):
        over = self.col + delta >= self.cols if delta > 0 else self.col + delta < 0
        return jnp.logical_and(self.has(delta), over)

    def copy(self, src, dst, delta):
        slot = len(self.copies)
        descriptor = pltpu.make_async_remote_copy(
            src, dst, self.send.at[slot], self.recv.at[slot],
            device_id=self.peer(delta), device_id_type=MESH,
        )
        self.copies.append(Copy(self, descriptor, delta))
        return self.copies[-1]


class Level:
    def __init__(self, n, t, r, bs, k, ref, columns, ops):
        self.n, self.t, self.r, self.bs, self.k = n, t, r, bs, k
        self.ref, self.columns, self.ops = ref, columns, ops
        self.base = ops.me * n
        self.scale = 1.0 / (k * bs)

    def weight_sums(self, b):
        w = self.ref["w"][b]
        return jnp.dot(jnp.ones((8, w.shape[0]), BF16), w, preferred_element_type=F32)

    def put_diagonal(self, b, total):
        degree = self.ref["deg"][pl.ds(b, 1), :]
        g = degree + total * self.scale
        self.ref["g"][b] = g
        self.ref["gi"][b] = DAMPING / g

    def spread(self, row):
        return jnp.broadcast_to(row, (self.r, self.bs))

    def put_hot(self, row, columns):
        size = 32
        index = lax.broadcasted_iota(jnp.int32, (size, self.bs), 0)
        away = (index - jnp.broadcast_to(row, (size, self.bs))).astype(jnp.int16)
        one, zero = jnp.ones((size, self.bs), BF16), jnp.zeros((size, self.bs), BF16)
        for low in range(0, self.t, size):
            hit = jnp.where(away == jnp.int16(-low), one, zero)
            self.ref["oh"][low : low + size, columns] = hit.astype(F8)

    def put_residual(self, columns, res, rel):
        rows = self.r
        out = self.ref["res"]
        zero = jnp.zeros_like(res)
        out[0:rows, columns] = jnp.where(rel < 0, res, zero).astype(BF16)
        out[rows : 2 * rows, columns] = jnp.where(rel == 0, res, zero).astype(BF16)
        out[2 * rows : 3 * rows, columns] = jnp.where(rel > 0, res, zero).astype(BF16)

    def restricted(self, res, hot):
        return lax.dot_general(
            res, hot, (((1,), (1,)), ((), ())), preferred_element_type=F32
        )


class Fine(Level):
    def __init__(self, *args):
        super().__init__(*args)
        ref, ops, n = self.ref, self.ops, self.n
        self.halo = []
        for i in range(4):
            vb = ref[f"vb{i}"]
            self.halo.append([
                ops.copy(vb.at[n - 2 : n], ref[f"lo{i}"].at[0:2], 1),
                ops.copy(vb.at[0:2], ref[f"hi{i}"].at[4:6], -1),
            ])
        self.prolong = [
            ops.copy(ref["uout"], ref["uin"].at[0], 1),
            ops.copy(ref["uout"], ref["uin"].at[1], -1),
        ]
        out, got = ref["rout"], ref["rin"]
        tiles = self.t // (2 * self.bs)
        last = tiles - 1
        self.tiles = [0, last] + list(range(1, last))
        self.restrict_copies = {}
        for j in self.tiles:
            at = slice(2 * j, 2 * j + 2)
            made = [
                ops.copy(out.at[2, at], got.at[0, at], 1),
                ops.copy(out.at[0, at], got.at[1, at], -1),
            ]
            if j == 0:
                made.append(ops.copy(out.at[1, at], ref["near"].at[1], -1))
                made.append(ops.copy(out.at[0, at], ref["far"].at[1], -2))
            if j == last:
                made.append(ops.copy(out.at[1, at], ref["near"].at[0], 1))
                made.append(ops.copy(out.at[2, at], ref["far"].at[0], 2))
            self.restrict_copies[j] = made

    def edges(self):
        return [0, 1, self.n - 2, self.n - 1]

    def inner(self):
        return 2, self.n - 2

    def row(self, name, b):
        return self.spread(self.ref[name][b, 0:1, :])

    def f(self, b):
        return self.ref["f"][b].astype(F32)

    def product(self, i, b, where):
        if where == "inner":
            buf, offset = self.ref[f"vb{i}"], self.base
        elif where == "low":
            buf, offset = self.ref[f"lo{i}"], self.base - 2
        else:
            buf, offset = self.ref[f"hi{i}"], self.base + self.n - 4
        top = buf.shape[0] - 1
        picked = [
            buf[jnp.clip(self.columns[k, b] - offset, 0, top)] for k in range(self.k)
        ]
        left = jnp.concatenate(picked, axis=1)
        return jnp.dot(left, self.ref["w"][b], preferred_element_type=F32) * self.scale

    def apply(self, i, body, meanwhile=None):
        grouped(*self.inner(), lambda b: self.product(i, b, "inner"), body)
        n = self.n
        self.ref[f"lo{i}"][2:6] = self.ref[f"vb{i}"][0:4]
        self.ref[f"hi{i}"][0:4] = self.ref[f"vb{i}"][n - 4 : n]
        if meanwhile is not None:
            meanwhile()
        wait(self.halo[i])
        made = [self.product(i, b, "low" if b < 2 else "high") for b in self.edges()]
        for b, product in zip(self.edges(), made):
            body(b, product)

    def start_block(self, b):
        self.ref["vb0"][b] = (self.row("gi", b) * self.f(b)).astype(BF16)

    def first_sweep(self, b, product):
        f, gi = self.f(b), self.row("gi", b)
        x0 = gi * f
        x = (1.0 - DAMPING) * x0 + gi * (f + product)
        self.ref["x"][b] = x
        self.ref["vb1"][b] = x.astype(BF16)

    def at(self, b):
        return pl.ds(pl.multiple_of(b * self.bs, self.bs), self.bs)

    def owner(self, b):
        return self.spread(self.ref["own"][pl.ds(b, 1), :] - self.ops.me)

    def residual(self, b, product):
        res = self.f(b) - self.row("g", b) * self.ref["x"][b] + product
        self.put_residual(self.at(b), res, self.owner(b))

    def make_onehot(self, b):
        self.put_hot(self.ref["slot"][pl.ds(b, 1), :], self.at(b))

    def restrict_inner(self):
        bs = self.bs
        inner = slice(2 * bs, (self.n - 2) * bs)
        for j in self.tiles:
            at = slice(2 * j * bs, (2 * j + 2) * bs)
            self.ref["part"][:, at] = self.restricted(
                self.ref["res"][:, inner], self.ref["oh"][at, inner]
            )

    def restrict(self):
        r, bs = self.r, self.bs
        ends = (slice(0, 2 * bs), slice((self.n - 2) * bs, self.n * bs))
        for j in self.tiles:
            at = slice(2 * j * bs, (2 * j + 2) * bs)
            value = self.ref["part"][:, at]
            for end in ends:
                value += self.restricted(self.ref["res"][:, end], self.ref["oh"][at, end])
            for half in range(2):
                b = 2 * j + half
                part = value[:, half * bs : (half + 1) * bs]
                for way in range(3):
                    self.ref["rout"][way, b] = part[way * r : (way + 1) * r].astype(BF16)
                self.ref["rown"][b] = part[r : 2 * r]
            start(self.restrict_copies[j])

    def received(self, below):
        for j in self.tiles:
            wait(self.restrict_copies[j])
        got, out = self.ref["rin"], self.ref["rout"]
        n = below.n
        for b in range(n):
            below.ref["f"][b] = self.ref["rown"][b] + got[0, b].astype(F32) + got[1, b].astype(F32)
        for side, way, first in ((0, 0, n - 2), (1, 2, 0)):
            for j in range(2):
                below.ref["fn"][side, j] = (
                    self.ref["near"][side, j].astype(F32)
                    + self.ref["far"][side, j].astype(F32)
                    + out[way, first + j].astype(F32)
                )

    def pair_columns(self, pair):
        return pl.ds(pl.multiple_of(pair * 2 * self.bs, 2 * self.bs), 2 * self.bs)

    def own_part(self, pair):
        return jnp.dot(
            self.ref["uout"][...], self.ref["oh"][:, self.pair_columns(pair)],
            preferred_element_type=F32,
        )

    def add_own(self, pair, value):
        for half in range(2):
            b = 2 * pair + half
            part = value[:, half * self.bs : (half + 1) * self.bs]
            self.ref["x"][b] = self.ref["x"][b] + jnp.where(self.owner(b) == 0, part, 0.0)

    def others_part(self, pair):
        left = jnp.concatenate([self.ref["uin"][0], self.ref["uin"][1]], axis=0)
        return jnp.dot(
            left, self.ref["oh"][:, self.pair_columns(pair)], preferred_element_type=F32
        )

    def add_others(self, pair, value):
        for half in range(2):
            b = 2 * pair + half
            at = slice(half * self.bs, (half + 1) * self.bs)
            rel = self.owner(b)
            x = self.ref["x"][b]
            x = x + jnp.where(rel < 0, value[0 : self.r, at], 0.0)
            x = x + jnp.where(rel > 0, value[self.r : 2 * self.r, at], 0.0)
            self.ref["x"][b] = x
            self.ref["vb2"][b] = x.astype(BF16)

    def sweep(self, i, out):
        def body(b, product):
            x = (1.0 - DAMPING) * self.ref["x"][b] + self.row("gi", b) * (self.f(b) + product)
            if out is None:
                self.ref["x"][b] = x
                self.ref[f"vb{i + 1}"][b] = x.astype(BF16)
            else:
                out[b] = x

        return body

    def up(self, out):
        start(self.prolong)
        pairs = self.n // 2
        grouped(0, pairs, self.own_part, self.add_own, 2)
        wait(self.prolong)
        ends = [0, pairs - 1]
        made = [self.others_part(pair) for pair in ends]
        for pair, value in zip(ends, made):
            self.add_others(pair, value)
        start(self.halo[2])
        grouped(1, pairs - 1, self.others_part, self.add_others, 2)
        self.apply(2, self.sweep(2, None))
        start(self.halo[3])
        self.apply(3, self.sweep(3, out))

    def clear_ends(self):
        for name, low, high in (("rin", 0, 1), ("uin", 0, 1), ("near", 0, 1), ("far", 0, 1)):
            ref = self.ref[name]
            for entry, missing in ((low, -2 if name == "far" else -1), (high, 2 if name == "far" else 1)):

                @pl.when(jnp.logical_not(self.ops.has(missing)))
                def _():
                    ref[entry] = jnp.zeros(ref.shape[1:], ref.dtype)


class Small(Level):
    def __init__(self, n, t, r, bs, k, ref, columns, ops, halo, weight_ways, degree_ways, send_ways):
        super().__init__(n, t, r, bs, k, ref, columns[0], ops)
        self.halo, self.m = halo, min(n, 2)
        self.other_columns = columns[1:]
        self.weight_ways, self.degree_ways, self.send_ways = weight_ways, degree_ways, send_ways
        ways = weight_ways
        self.tables, self.weights = [], []
        for at, d in enumerate(ways):
            self.tables.append(ops.copy(ref["own"], ref["ownn"].at[at], -d))
            self.tables.append(ops.copy(ref["slot"], ref["slotn"].at[at], -d))
            self.tables.append(ops.copy(columns[0], columns[1 + at], -d))
        for at, d in enumerate(degree_ways):
            self.tables.append(ops.copy(ref["g"].at[self.edge(d)], ref["gn"].at[at], -d))
        for j in range(self.m):
            for rows in range(k):
                part = slice(rows * bs, (rows + 1) * bs)
                group = []
                for at, d in enumerate(ways):
                    source = self.edge(d).start + j
                    group.append(ops.copy(ref["w"].at[source, part], ref["wn"].at[at, j, part], -d))
                self.weights.append(group)
        self.sends = [
            ops.copy(ref["uout"], ref["uin"].at[at], -d) for at, d in self.far_first(send_ways)
        ]

    def far_first(self, ways):
        return sorted(enumerate(ways), key=lambda pair: -abs(pair[1]))

    def edge(self, d):
        return slice(self.n - self.m, self.n) if d < 0 else slice(0, self.m)

    def place(self, b):
        d = b // self.n
        j = b - d * self.n
        return d, j, j - self.edge(d).start

    def column(self, b, k):
        d, j, _ = self.place(b)
        table = self.columns if d == 0 else self.other_columns[self.weight_ways.index(d)]
        return table[j, k] if self.n < 4 else table[k, j]

    def w(self, b):
        d, j, e = self.place(b)
        return self.ref["w"][j] if d == 0 else self.ref["wn"][self.weight_ways.index(d), e]

    def row(self, name, b):
        d, j, e = self.place(b)
        if d == 0:
            return self.spread(self.ref[name][j, 0:1, :])
        return self.spread(self.ref[name + "n"][self.degree_ways.index(d), e, 0:1, :])

    def f(self, b):
        d, j, e = self.place(b)
        if d == 0:
            return self.ref["f"][j]
        return self.ref["fn"][self.degree_ways.index(d), e].astype(F32)

    def table(self, name, b):
        d, j, _ = self.place(b)
        if d == 0:
            return self.ref[name][j : j + 1, :]
        return self.ref[name + "n"][self.weight_ways.index(d), j : j + 1, :]

    def owner(self, b):
        return self.spread(self.table("own", b) - self.ops.me)

    def invert(self):
        for at in range(len(self.degree_ways)):
            for e in range(self.m):
                self.ref["gin"][at, e] = DAMPING / self.ref["gn"][at, e]

    def make_onehots(self, reach):
        for b in range(-reach, self.n + reach):
            at = (b + reach) * self.bs
            self.put_hot(self.table("slot", b), slice(at, at + self.bs))

    def product(self, i, b):
        buf = self.ref[f"vb{i}"]
        offset = self.base - self.halo
        top = buf.shape[0] - 1
        picked = [
            buf[jnp.clip(self.column(b, k) - offset, 0, top)] for k in range(self.k)
        ]
        left = jnp.concatenate(picked, axis=1)
        return jnp.dot(left, self.w(b), preferred_element_type=F32) * self.scale

    def apply(self, i, blocks, body, size=6):
        blocks = list(blocks)
        for low in range(0, len(blocks), size):
            group = blocks[low : low + size]
            made = [self.product(i, b) for b in group]
            for b, product in zip(group, made):
                body(b, product)

    def start_blocks(self, low, high):
        for b in range(low, high):
            self.ref["vb0"][b + self.halo] = (self.row("gi", b) * self.f(b)).astype(BF16)

    def first_sweep(self, b, product):
        f, gi = self.f(b), self.row("gi", b)
        x0 = gi * f
        x = (1.0 - DAMPING) * x0 + gi * (f + product)
        self.ref["x"][b + self.halo] = x
        self.ref["vb1"][b + self.halo] = x.astype(BF16)

    def residual_of(self, b, product):
        return self.f(b) - self.row("g", b) * self.ref["x"][b + self.halo] + product

    def add_correction(self, reach):
        bs, r = self.bs, self.r
        corrections = {0: self.ref["uout"]}
        for at, d in enumerate(self.send_ways):
            corrections[d] = self.ref["uin"].at[at]
        for b in range(-reach, self.n + reach, 2):
            d, _, _ = self.place(b)
            left = jnp.concatenate([corrections[d + way][...] for way in (-1, 0, 1)], axis=0)
            at = (b + reach) * bs
            value = jnp.dot(left, self.ref["oh"][:, at : at + 2 * bs], preferred_element_type=F32)
            for half in range(2):
                part = value[:, half * bs : (half + 1) * bs]
                rel = self.owner(b + half) - d
                low, own, high = (part[way * r : (way + 1) * r] for way in range(3))
                add = jnp.where(rel == 0, own, jnp.where(rel < 0, low, high))
                x = self.ref["x"][b + half + self.halo] + add
                self.ref["x"][b + half + self.halo] = x
                self.ref["vb2"][b + half + self.halo] = x.astype(BF16)

    def sweep(self, i, out=None):
        def body(b, product):
            h = self.halo
            x = (1.0 - DAMPING) * self.ref["x"][b + h] + self.row("gi", b) * (self.f(b) + product)
            if out is None:
                self.ref["x"][b + h] = x
                self.ref[f"vb{i + 1}"][b + h] = x.astype(BF16)
            else:
                out(b, x)

        return body

    def clear_ends(self):
        for at, d in enumerate(self.weight_ways):

            @pl.when(jnp.logical_not(self.ops.has(d)))
            def _():
                self.ref["ownn"][at] = jnp.full(self.ref["ownn"].shape[1:], -8, jnp.int32)
                self.ref["slotn"][at] = jnp.zeros(self.ref["slotn"].shape[1:], jnp.int32)
                self.ref["wn"][at] = jnp.zeros(self.ref["wn"].shape[1:], BF16)
                columns = self.other_columns[at]
                for i in range(columns.shape[0]):
                    for j in range(columns.shape[1]):
                        columns[i, j] = 0

        for at, d in enumerate(self.degree_ways):

            @pl.when(jnp.logical_not(self.ops.has(d)))
            def _():
                self.ref["gn"][at] = jnp.ones(self.ref["gn"].shape[1:], F32)
                self.ref["fn"][at] = jnp.zeros(self.ref["fn"].shape[1:], self.ref["fn"].dtype)

        for at, d in enumerate(self.send_ways):

            @pl.when(jnp.logical_not(self.ops.has(d)))
            def _():
                self.ref["uin"][at] = jnp.zeros(self.ref["uin"].shape[1:], BF16)


class Second(Small):
    def __init__(self, *args):
        super().__init__(*args, 4, (-1, 1), (-1, 1), (-2, -1, 1, 2))
        ref, ops, n, h = self.ref, self.ops, self.n, self.halo
        vb, got = ref["vb1"], ref["vin"]
        own = lambda low, high: vb.at[h + low : h + high]
        self.halo_near = [
            ops.copy(own(n - 2, n), got.at[0, 2:4], 1), ops.copy(own(0, 2), got.at[1, 0:2], -1)
        ]
        self.halo_far = [
            ops.copy(own(n - 4, n - 2), got.at[0, 0:2], 1), ops.copy(own(2, 4), got.at[1, 2:4], -1)
        ]
        self.restrict_copies = [
            ops.copy(ref["rout"].at[1], ref["rin"].at[0], 1),
            ops.copy(ref["rout"].at[0], ref["rin"].at[1], -1),
        ]

    def residual(self, b, product):
        at = slice(b * self.bs, (b + 1) * self.bs)
        self.put_residual(at, self.residual_of(b, product), self.owner(b))

    def down(self, below, meanwhile):
        n, h, r, bs = self.n, self.halo, self.r, self.bs
        self.start_blocks(-2, n + 2)
        edges = [0, 1, n - 2, n - 1]
        self.apply(0, edges, self.first_sweep)
        start(self.halo_near)
        self.apply(0, range(2, n - 2), self.first_sweep)
        start(self.halo_far)
        meanwhile()
        self.apply(1, range(2, n - 2), self.residual)
        wait(self.halo_near)
        self.ref["vb1"][h - 2 : h] = self.ref["vin"][0, 2:4]
        self.ref["vb1"][h + n : h + n + 2] = self.ref["vin"][1, 0:2]
        self.apply(1, edges, self.residual)
        reach = 4
        own = slice(reach * bs, (reach + n) * bs)
        value = self.restricted(self.ref["res"][...], self.ref["oh"][:, own])
        for b in range(below.n):
            at = slice(b * bs, (b + 1) * bs)
            self.ref["rout"][0, b] = value[0:r, at].astype(BF16)
            self.ref["rout"][1, b] = value[2 * r : 3 * r, at].astype(BF16)
        start(self.restrict_copies)
        for b in range(below.n):
            self.ref["rown"][b] = value[r : 2 * r, b * bs : (b + 1) * bs]

    def received(self, below):
        wait(self.restrict_copies)
        got = self.ref["rin"]
        for b in range(below.n):
            f = self.ref["rown"][b] + got[0, b].astype(F32) + got[1, b].astype(F32)
            below.ref["f"][b] = f
            below.ref["fout"][b] = f.astype(BF16)

    def finish(self, out):
        n, h = self.n, self.halo
        wait(self.halo_far)
        for j in range(4):
            self.ref["x"][h - 4 + j] = self.ref["vin"][0, j].astype(F32)
            self.ref["x"][h + n + j] = self.ref["vin"][1, j].astype(F32)
        wait(self.sends)
        self.add_correction(4)
        for group in self.weights:
            wait(group)
        self.apply(2, range(-2, n + 2), self.sweep(2))
        self.apply(3, range(n), self.sweep(3, out))

    def clear_ends(self):
        super().clear_ends()
        for name in ("rin", "vin"):
            for at, d in ((0, -1), (1, 1)):

                @pl.when(jnp.logical_not(self.ops.has(d)))
                def _():
                    self.ref[name][at] = jnp.zeros(self.ref[name].shape[1:], BF16)


class Third(Small):
    def __init__(self, *args):
        super().__init__(*args, 6, (-2, -1, 1, 2), (-3, -2, -1, 1, 2, 3), (-3, -2, -1, 1, 2, 3))
        ref, ops = self.ref, self.ops
        self.sources = [
            ops.copy(ref["fout"], ref["fn"].at[at], -d)
            for at, d in self.far_first(self.degree_ways)
        ]

    def down(self, into):
        n, bs = self.n, self.bs
        wait(self.sources)
        self.start_blocks(-6, n + 6)
        for group in self.weights:
            wait(group)
        self.apply(0, range(-4, n + 4), self.first_sweep)

        def residual(b, product):
            res = self.residual_of(b, product)
            at = (b + 2) * bs
            kept = jnp.where(self.owner(b) == 0, res, jnp.zeros_like(res))
            self.ref["res"][:, at : at + bs] = kept.astype(BF16)

        self.apply(1, range(-2, n + 2), residual)
        near = slice(2 * bs, (n + 6) * bs)
        into(self.restricted(self.ref["res"][...], self.ref["oh"][:, near]))

    def finish(self, out):
        n = self.n
        wait(self.sends)
        self.add_correction(4)
        self.apply(2, range(-2, n + 2), self.sweep(2))
        self.apply(3, range(n), self.sweep(3, out))


LEVEL_HBM = ("w", "deg", "own", "slot")
SHARED = ("w", "deg", "own", "slot", "g", "gi", "x", "vb0", "vb1", "vb2", "vb3", "res", "oh", "uout", "uin")
FINE = SHARED + (
    "lo0", "lo1", "lo2", "lo3", "hi0", "hi1", "hi2", "hi3", "rout", "rin", "rown", "near", "far", "part",
)
SMALL = SHARED + ("f", "fn", "wn", "ownn", "slotn", "gn", "gin")
SECOND = SMALL + ("rout", "rin", "rown", "vin")
THIRD = SMALL + ("fout",)


def kernel(sizes, rhs_count, bs, k, *refs):
    refs = list(refs)
    take = lambda count: [refs.pop(0) for _ in range(count)]
    rhs_hbm, inverse_hbm = take(2)
    columns_hbm, hbm = [], []
    for _ in sizes:
        columns_hbm.append(refs.pop(0))
        hbm.append(dict(zip(LEVEL_HBM, take(4))))
    (out,) = take(1)
    scratch = [dict(zip(names, take(len(names)))) for names in (FINE, SECOND, THIRD)]
    columns = [take(1), take(3), take(5)]
    rhs, inverse, gathered = take(3)
    send, recv, gather_send, gather_recv, local = take(5)

    ops = Ops(send, recv)
    scratch[0]["f"] = rhs
    (n0, t0), (n1, t1), (n2, t2) = sizes
    fine = Fine(n0, t0, rhs_count, bs, k, scratch[0], columns[0][0], ops)
    second = Second(n1, t1, rhs_count, bs, k, scratch[1], columns[1], ops)
    third = Third(n2, t2, rhs_count, bs, k, scratch[2], columns[2], ops)
    levels = [fine, second, third]

    loads = []

    def load(src, dst):
        copy = pltpu.make_async_copy(src, dst, local.at[len(loads)])
        loads.append(copy)
        copy.start()
        return copy

    n = fine.n
    early = []
    for at in (slice(0, 2), slice(n - 2, n)):
        early.append(load(hbm[0]["w"].at[at], scratch[0]["w"].at[at]))
    early.append(load(hbm[0]["deg"], scratch[0]["deg"]))
    early.append(load(rhs_hbm, rhs))
    for level in range(3):
        early.append(load(columns_hbm[level], columns[level][0]))
    heavy = load(hbm[2]["w"], scratch[2]["w"])
    middle = load(hbm[0]["w"].at[2 : n - 2], scratch[0]["w"].at[2 : n - 2])
    later = [load(hbm[0][name], scratch[0][name]) for name in ("own", "slot")]
    for position in (1, 2):
        names = LEVEL_HBM[position - 1 :]
        later += [load(hbm[position][name], scratch[position][name]) for name in names]
    last = load(inverse_hbm, inverse)

    barrier = pltpu.get_barrier_semaphore()
    expected = ops.cols - 1
    for delta in (-3, -2, -1, 1, 2, 3):
        outside = ops.across(delta)
        pl.when(outside)(
            lambda: pl.semaphore_signal(
                barrier, inc=1, device_id=ops.peer(delta), device_id_type=MESH
            )
        )
        expected = expected + outside.astype(jnp.int32)
    for step in range(1, ops.cols):
        peer = lax.rem(ops.col + step, ops.cols)
        pl.semaphore_signal(barrier, inc=1, device_id=(ops.row, peer), device_id_type=MESH)
    for level in levels:
        level.clear_ends()
    for copy in early:
        copy.wait()

    def diagonal_and_start(b, total):
        fine.put_diagonal(b, total)
        fine.start_block(b)

    made = [fine.weight_sums(b) for b in fine.edges()]
    for b, total in zip(fine.edges(), made):
        diagonal_and_start(b, total)
    pl.semaphore_wait(barrier, expected)
    start(fine.halo[0])
    third_weights = Slots(third.weights, THIRD_SLOTS)
    second_weights = Slots(second.weights, SECOND_SLOTS)
    heavy.wait()
    third_weights.send()
    middle.wait()
    grouped(*fine.inner(), fine.weight_sums, diagonal_and_start)
    for copy in later:
        copy.wait()
    for level in (second, third):
        grouped(0, level.n, level.weight_sums, level.put_diagonal, 8)
    start(second.tables)
    start(third.tables)
    loop(0, n, fine.make_onehot, 2)
    fine.apply(0, fine.first_sweep)
    start(fine.halo[1])
    third_weights.send()
    fine.apply(1, fine.residual, fine.restrict_inner)
    fine.restrict()
    for level in (second, third):
        wait(level.tables)
        level.invert()
        level.make_onehots(4)
    fine.received(second)

    second.down(third, third_weights.send)
    third_weights.send()
    second_weights.send()
    second.received(third)
    start(third.sources)
    second_weights.send()

    def into_coarse(value):
        gathered[ops.col] = value.astype(BF16)

    third.down(into_coarse)

    sends = []
    for step in range(1, ops.cols):
        peer = lax.rem(ops.col + step, ops.cols)
        copy = pltpu.make_async_remote_copy(
            gathered.at[ops.col], gathered.at[ops.col],
            gather_send.at[step - 1], gather_recv.at[step - 1],
            device_id=(ops.row, peer), device_id_type=MESH,
        )
        copy.start()
        sends.append(copy)
    second_weights.send()
    last.wait()
    for step in range(1, ops.cols):
        source = lax.rem(ops.col + ops.cols - step, ops.cols)
        pltpu.make_async_remote_copy(
            gathered.at[source], gathered.at[source],
            gather_send.at[step - 1], gather_recv.at[step - 1],
            device_id=(ops.row, source), device_id_type=MESH,
        ).wait_recv()
    everything = jnp.concatenate([gathered[p] for p in range(ops.cols)], axis=1)
    solved = lax.dot_general(
        everything, inverse[...], (((1,), (1,)), ((), ())), preferred_element_type=F32
    )
    third.ref["uout"][...] = solved.astype(BF16)
    start(third.sends)
    second_weights.send()

    def into_coarse_vector(level):
        def put(b, x):
            level.ref["uout"][:, b * bs : (b + 1) * bs] = x.astype(BF16)

        return put

    third.finish(into_coarse_vector(second))
    start(second.sends)
    second.finish(into_coarse_vector(fine))
    fine.up(out)
    for copy in ops.copies:
        copy.drain()
    for copy in sends:
        copy.wait_send()


def on_device(
    right_sides,
    weights_fine, columns_fine, degree_fine, owners_fine, slots_fine,
    weights_second, columns_second, degree_second, owners_second, slots_second,
    weights_third, columns_third, degree_third, owners_third, slots_third,
    coarse_inverse,
):
    n0, r, bs = right_sides.shape
    n1, n2 = weights_second.shape[0], weights_third.shape[0]
    k = weights_fine.shape[1]
    c3, m3 = coarse_inverse.shape
    cols = lax.axis_size("col")
    sizes = ((n0, n1 * bs), (n1, n2 * bs), (n2, c3))
    merged = lambda w: w.reshape(w.shape[0], k * bs, bs)
    args = [right_sides, coarse_inverse]
    for w, c, d, o, s in (
        (weights_fine, columns_fine, degree_fine, owners_fine, slots_fine),
        (weights_second, columns_second, degree_second, owners_second, slots_second),
        (weights_third, columns_third, degree_third, owners_third, slots_third),
    ):
        args += [c.T if c.shape[0] >= 4 else c, merged(w), d, o, s]
    specs = [pl.BlockSpec(memory_space=pltpu.HBM)] * len(args)
    vmem = pltpu.VMEM
    vector = lambda *lead: vmem((*lead, r, bs), BF16)

    def shared(n, t, window, ways, res, hot):
        return [
            vmem((n, k * bs, bs), BF16),
            vmem((n, bs), F32),
            vmem((n, bs), jnp.int32),
            vmem((n, bs), jnp.int32),
            vmem((n, 8, bs), F32),
            vmem((n, 8, bs), F32),
            vmem((window, r, bs), F32),
            *[vector(window)] * 4,
            vmem((res[0] * r, res[1] * bs), BF16),
            vmem((t, hot * bs), F8),
            vmem((r, t), BF16),
            vmem((ways, r, t), BF16),
        ]

    def small(n, weights, degrees, source):
        m = min(n, 2)
        return [
            vmem((n, r, bs), F32),
            vmem((degrees, m, r, bs), source),
            vmem((weights, m, k * bs, bs), BF16),
            vmem((weights, n, bs), jnp.int32),
            vmem((weights, n, bs), jnp.int32),
            vmem((degrees, m, 8, bs), F32),
            vmem((degrees, m, 8, bs), F32),
        ]

    scratch = shared(n0, n1 * bs, n0, 2, (3, n0), n0)
    scratch += [vector(6)] * 8
    scratch += [vector(3, n1), vector(2, n1), vmem((n1, r, bs), F32), vector(2, 2), vector(2, 2)]
    scratch += [vmem((3 * r, n1 * bs), F32)]
    scratch += shared(n1, n2 * bs, n1 + 8, 4, (3, n1), n1 + 8)
    scratch += small(n1, 2, 2, F32)
    scratch += [vector(2, n2), vector(2, n2), vmem((n2, r, bs), F32), vector(2, 4)]
    scratch += shared(n2, c3, n2 + 12, 6, (1, n2 + 4), n2 + 8)
    scratch += small(n2, 4, 6, BF16)
    scratch += [vector(n2)]
    scratch += [pltpu.SMEM((k, n0), jnp.int32)]
    scratch += [pltpu.SMEM((k, n1), jnp.int32)] * 3
    scratch += [pltpu.SMEM((n2, k), jnp.int32)] * 5
    scratch += [
        vector(n0),
        vmem((c3, m3), BF16),
        vmem((cols, r, c3), BF16),
        pltpu.SemaphoreType.DMA((140,)),
        pltpu.SemaphoreType.DMA((140,)),
        pltpu.SemaphoreType.DMA((cols,)),
        pltpu.SemaphoreType.DMA((cols,)),
        pltpu.SemaphoreType.DMA((24,)),
    ]
    return pl.pallas_call(
        functools.partial(kernel, sizes, r, bs, k),
        out_shape=jax.ShapeDtypeStruct((n0, r, bs), F32),
        in_specs=specs,
        out_specs=pl.BlockSpec(memory_space=pltpu.VMEM),
        scratch_shapes=scratch,
        compiler_params=pltpu.CompilerParams(
            collective_id=0, has_side_effects=True, vmem_limit_bytes=48 * 1024 * 1024
        ),
        name="vcycle",
    )(*[pltpu.with_memory_space_constraint(a, pltpu.HBM) for a in args])


def solution(mesh):
    whole = ("row", "col")
    vector, matrix, table = P(whole, None, None), P(whole, None, None, None), P(whole, None)
    level = (matrix, table, table, table, table)
    return jax.shard_map(
        on_device,
        mesh=mesh,
        in_specs=(vector, *level, *level, *level, table),
        out_specs=vector,
        check_vma=False,
    )
```

```python
import functools

import jax
import jax.numpy as jnp
from jax import lax
from jax.experimental import pallas as pl
from jax.experimental.pallas import tpu as pltpu
from jax.sharding import PartitionSpec as P

F32 = jnp.float32
BF16 = jnp.bfloat16
F8 = jnp.float8_e4m3fn
MESH = pl.DeviceIdType.MESH
DAMPING = 0.8
THIRD_SLOTS = (2, 1, 2, 1)
SECOND_SLOTS = (1, 1, 2, 2)


def loop(low, high, body, unroll=4):
    count = high - low
    if count <= 0:
        return
    while count % unroll:
        unroll -= 1

    if count == unroll:
        for inner in range(count):
            body(low + inner)
        return

    def step(outer, carry):
        for inner in range(unroll):
            body(low + outer * unroll + inner)
        return carry

    lax.fori_loop(0, count // unroll, step, 0)


def grouped(low, high, first, then, unroll=7):
    count = high - low
    if count <= 0:
        return
    while count % unroll:
        unroll -= 1

    def group(start):
        made = [first(start + inner) for inner in range(unroll)]
        for inner in range(unroll):
            then(start + inner, made[inner])

    if count == unroll:
        group(low)
        return

    def step(outer, carry):
        group(low + outer * unroll)
        return carry

    lax.fori_loop(0, count // unroll, step, 0)


class Copy:
    def __init__(self, ops, descriptor, delta):
        self.ops, self.descriptor, self.delta = ops, descriptor, delta

    def start(self):
        pl.when(self.ops.has(self.delta))(lambda: self.descriptor.start())

    def wait(self):
        pl.when(self.ops.has(-self.delta))(lambda: self.descriptor.wait_recv())

    def drain(self):
        pl.when(self.ops.has(self.delta))(lambda: self.descriptor.wait_send())


class Slots:
    def __init__(self, groups, counts):
        self.groups, self.counts = list(groups), list(counts)

    def send(self):
        for _ in range(self.counts.pop(0)):
            start(self.groups.pop(0))


def start(copies):
    for copy in copies:
        copy.start()


def wait(copies):
    for copy in copies:
        copy.wait()


class Ops:
    def __init__(self, send, recv):
        self.send, self.recv = send, recv
        self.rows, self.cols = lax.axis_size("row"), lax.axis_size("col")
        self.total = self.rows * self.cols
        self.row, self.col = lax.axis_index("row"), lax.axis_index("col")
        self.me = self.row * self.cols + self.col
        self.copies = []

    def has(self, delta):
        return self.me < self.total - delta if delta > 0 else self.me >= -delta

    def peer(self, delta):
        index = jnp.clip(self.me + delta, 0, self.total - 1)
        return (index // self.cols, index % self.cols)

    def across(self, delta):
        over = self.col + delta >= self.cols if delta > 0 else self.col + delta < 0
        return jnp.logical_and(self.has(delta), over)

    def copy(self, src, dst, delta):
        slot = len(self.copies)
        descriptor = pltpu.make_async_remote_copy(
            src, dst, self.send.at[slot], self.recv.at[slot],
            device_id=self.peer(delta), device_id_type=MESH,
        )
        self.copies.append(Copy(self, descriptor, delta))
        return self.copies[-1]


class Level:
    def __init__(self, n, t, r, bs, k, ref, columns, ops):
        self.n, self.t, self.r, self.bs, self.k = n, t, r, bs, k
        self.ref, self.columns, self.ops = ref, columns, ops
        self.base = ops.me * n
        self.scale = 1.0 / (k * bs)

    def weight_sums(self, b):
        w = self.ref["w"][b]
        return jnp.dot(jnp.ones((8, w.shape[0]), BF16), w, preferred_element_type=F32)

    def put_diagonal(self, b, total):
        degree = self.ref["deg"][pl.ds(b, 1), :]
        g = degree + total * self.scale
        self.ref["g"][b] = g
        self.ref["gi"][b] = DAMPING / g

    def spread(self, row):
        return jnp.broadcast_to(row, (self.r, self.bs))

    def put_hot(self, row, columns):
        size = 32
        index = lax.broadcasted_iota(jnp.int32, (size, self.bs), 0)
        away = (index - jnp.broadcast_to(row, (size, self.bs))).astype(jnp.int16)
        one, zero = jnp.ones((size, self.bs), BF16), jnp.zeros((size, self.bs), BF16)
        for low in range(0, self.t, size):
            hit = jnp.where(away == jnp.int16(-low), one, zero)
            self.ref["oh"][low : low + size, columns] = hit.astype(F8)

    def put_residual(self, columns, res, rel):
        rows = self.r
        out = self.ref["res"]
        zero = jnp.zeros_like(res)
        out[0:rows, columns] = jnp.where(rel < 0, res, zero).astype(BF16)
        out[rows : 2 * rows, columns] = jnp.where(rel == 0, res, zero).astype(BF16)
        out[2 * rows : 3 * rows, columns] = jnp.where(rel > 0, res, zero).astype(BF16)

    def restricted(self, res, hot):
        return lax.dot_general(
            res, hot, (((1,), (1,)), ((), ())), preferred_element_type=F32
        )


class Fine(Level):
    def __init__(self, *args):
        super().__init__(*args)
        ref, ops, n = self.ref, self.ops, self.n
        self.halo = []
        for i in range(4):
            vb = ref[f"vb{i}"]
            self.halo.append([
                ops.copy(vb.at[n - 2 : n], ref[f"lo{i}"].at[0:2], 1),
                ops.copy(vb.at[0:2], ref[f"hi{i}"].at[4:6], -1),
            ])
        self.prolong = [
            ops.copy(ref["uout"], ref["uin"].at[0], 1),
            ops.copy(ref["uout"], ref["uin"].at[1], -1),
        ]
        out, got = ref["rout"], ref["rin"]
        tiles = self.t // (2 * self.bs)
        last = tiles - 1
        self.tiles = [0, last] + list(range(1, last))
        self.restrict_copies = {}
        for j in self.tiles:
            at = slice(2 * j, 2 * j + 2)
            made = [
                ops.copy(out.at[2, at], got.at[0, at], 1),
                ops.copy(out.at[0, at], got.at[1, at], -1),
            ]
            if j == 0:
                made.append(ops.copy(out.at[1, at], ref["near"].at[1], -1))
                made.append(ops.copy(out.at[0, at], ref["far"].at[1], -2))
            if j == last:
                made.append(ops.copy(out.at[1, at], ref["near"].at[0], 1))
                made.append(ops.copy(out.at[2, at], ref["far"].at[0], 2))
            self.restrict_copies[j] = made

    def edges(self):
        return [0, 1, self.n - 2, self.n - 1]

    def inner(self):
        return 2, self.n - 2

    def row(self, name, b):
        return self.spread(self.ref[name][b, 0:1, :])

    def f(self, b):
        return self.ref["f"][b].astype(F32)

    def product(self, i, b, where):
        if where == "inner":
            buf, offset = self.ref[f"vb{i}"], self.base
        elif where == "low":
            buf, offset = self.ref[f"lo{i}"], self.base - 2
        else:
            buf, offset = self.ref[f"hi{i}"], self.base + self.n - 4
        top = buf.shape[0] - 1
        picked = [
            buf[jnp.clip(self.columns[k, b] - offset, 0, top)] for k in range(self.k)
        ]
        left = jnp.concatenate(picked, axis=1)
        return jnp.dot(left, self.ref["w"][b], preferred_element_type=F32) * self.scale

    def apply(self, i, body, meanwhile=None):
        grouped(*self.inner(), lambda b: self.product(i, b, "inner"), body)
        n = self.n
        self.ref[f"lo{i}"][2:6] = self.ref[f"vb{i}"][0:4]
        self.ref[f"hi{i}"][0:4] = self.ref[f"vb{i}"][n - 4 : n]
        if meanwhile is not None:
            meanwhile()
        wait(self.halo[i])
        made = [self.product(i, b, "low" if b < 2 else "high") for b in self.edges()]
        for b, product in zip(self.edges(), made):
            body(b, product)

    def start_block(self, b):
        self.ref["vb0"][b] = (self.row("gi", b) * self.f(b)).astype(BF16)

    def first_sweep(self, b, product):
        f, gi = self.f(b), self.row("gi", b)
        x0 = gi * f
        x = (1.0 - DAMPING) * x0 + gi * (f + product)
        self.ref["x"][b] = x
        self.ref["vb1"][b] = x.astype(BF16)

    def at(self, b):
        return pl.ds(pl.multiple_of(b * self.bs, self.bs), self.bs)

    def owner(self, b):
        return self.spread(self.ref["own"][pl.ds(b, 1), :] - self.ops.me)

    def residual(self, b, product):
        res = self.f(b) - self.row("g", b) * self.ref["x"][b] + product
        self.put_residual(self.at(b), res, self.owner(b))

    def make_onehot(self, b):
        self.put_hot(self.ref["slot"][pl.ds(b, 1), :], self.at(b))

    def restrict_inner(self):
        bs = self.bs
        inner = slice(2 * bs, (self.n - 2) * bs)
        for j in self.tiles:
            at = slice(2 * j * bs, (2 * j + 2) * bs)
            self.ref["part"][:, at] = self.restricted(
                self.ref["res"][:, inner], self.ref["oh"][at, inner]
            )

    def restrict(self):
        r, bs = self.r, self.bs
        ends = (slice(0, 2 * bs), slice((self.n - 2) * bs, self.n * bs))
        for j in self.tiles:
            at = slice(2 * j * bs, (2 * j + 2) * bs)
            value = self.ref["part"][:, at]
            for end in ends:
                value += self.restricted(self.ref["res"][:, end], self.ref["oh"][at, end])
            for half in range(2):
                b = 2 * j + half
                part = value[:, half * bs : (half + 1) * bs]
                for way in range(3):
                    self.ref["rout"][way, b] = part[way * r : (way + 1) * r].astype(BF16)
                self.ref["rown"][b] = part[r : 2 * r]
            start(self.restrict_copies[j])

    def received(self, below):
        for j in self.tiles:
            wait(self.restrict_copies[j])
        got, out = self.ref["rin"], self.ref["rout"]
        n = below.n
        for b in range(n):
            below.ref["f"][b] = self.ref["rown"][b] + got[0, b].astype(F32) + got[1, b].astype(F32)
        for side, way, first in ((0, 0, n - 2), (1, 2, 0)):
            for j in range(2):
                below.ref["fn"][side, j] = (
                    self.ref["near"][side, j].astype(F32)
                    + self.ref["far"][side, j].astype(F32)
                    + out[way, first + j].astype(F32)
                )

    def pair_columns(self, pair):
        return pl.ds(pl.multiple_of(pair * 2 * self.bs, 2 * self.bs), 2 * self.bs)

    def own_part(self, pair):
        return jnp.dot(
            self.ref["uout"][...], self.ref["oh"][:, self.pair_columns(pair)],
            preferred_element_type=F32,
        )

    def add_own(self, pair, value):
        for half in range(2):
            b = 2 * pair + half
            part = value[:, half * self.bs : (half + 1) * self.bs]
            self.ref["x"][b] = self.ref["x"][b] + jnp.where(self.owner(b) == 0, part, 0.0)

    def others_part(self, pair):
        left = jnp.concatenate([self.ref["uin"][0], self.ref["uin"][1]], axis=0)
        return jnp.dot(
            left, self.ref["oh"][:, self.pair_columns(pair)], preferred_element_type=F32
        )

    def add_others(self, pair, value):
        for half in range(2):
            b = 2 * pair + half
            at = slice(half * self.bs, (half + 1) * self.bs)
            rel = self.owner(b)
            x = self.ref["x"][b]
            x = x + jnp.where(rel < 0, value[0 : self.r, at], 0.0)
            x = x + jnp.where(rel > 0, value[self.r : 2 * self.r, at], 0.0)
            self.ref["x"][b] = x
            self.ref["vb2"][b] = x.astype(BF16)

    def sweep(self, i, out):
        def body(b, product):
            x = (1.0 - DAMPING) * self.ref["x"][b] + self.row("gi", b) * (self.f(b) + product)
            if out is None:
                self.ref["x"][b] = x
                self.ref[f"vb{i + 1}"][b] = x.astype(BF16)
            else:
                out[b] = x

        return body

    def up(self, out):
        start(self.prolong)
        pairs = self.n // 2
        grouped(0, pairs, self.own_part, self.add_own, 2)
        wait(self.prolong)
        ends = [0, pairs - 1]
        made = [self.others_part(pair) for pair in ends]
        for pair, value in zip(ends, made):
            self.add_others(pair, value)
        start(self.halo[2])
        grouped(1, pairs - 1, self.others_part, self.add_others, 2)
        self.apply(2, self.sweep(2, None))
        start(self.halo[3])
        self.apply(3, self.sweep(3, out))

    def clear_ends(self):
        for name, low, high in (("rin", 0, 1), ("uin", 0, 1), ("near", 0, 1), ("far", 0, 1)):
            ref = self.ref[name]
            for entry, missing in ((low, -2 if name == "far" else -1), (high, 2 if name == "far" else 1)):

                @pl.when(jnp.logical_not(self.ops.has(missing)))
                def _():
                    ref[entry] = jnp.zeros(ref.shape[1:], ref.dtype)


class Small(Level):
    def __init__(self, n, t, r, bs, k, ref, columns, ops, halo, weight_ways, degree_ways, send_ways):
        super().__init__(n, t, r, bs, k, ref, columns[0], ops)
        self.halo, self.m = halo, min(n, 2)
        self.other_columns = columns[1:]
        self.weight_ways, self.degree_ways, self.send_ways = weight_ways, degree_ways, send_ways
        ways = weight_ways
        self.tables, self.weights = [], []
        for at, d in enumerate(ways):
            self.tables.append(ops.copy(ref["own"], ref["ownn"].at[at], -d))
            self.tables.append(ops.copy(ref["slot"], ref["slotn"].at[at], -d))
            self.tables.append(ops.copy(columns[0], columns[1 + at], -d))
        for at, d in enumerate(degree_ways):
            self.tables.append(ops.copy(ref["g"].at[self.edge(d)], ref["gn"].at[at], -d))
        for j in range(self.m):
            for rows in range(k):
                part = slice(rows * bs, (rows + 1) * bs)
                group = []
                for at, d in enumerate(ways):
                    source = self.edge(d).start + j
                    group.append(ops.copy(ref["w"].at[source, part], ref["wn"].at[at, j, part], -d))
                self.weights.append(group)
        self.sends = [
            ops.copy(ref["uout"], ref["uin"].at[at], -d) for at, d in self.far_first(send_ways)
        ]

    def far_first(self, ways):
        return sorted(enumerate(ways), key=lambda pair: -abs(pair[1]))

    def edge(self, d):
        return slice(self.n - self.m, self.n) if d < 0 else slice(0, self.m)

    def place(self, b):
        d = b // self.n
        j = b - d * self.n
        return d, j, j - self.edge(d).start

    def column(self, b, k):
        d, j, _ = self.place(b)
        table = self.columns if d == 0 else self.other_columns[self.weight_ways.index(d)]
        return table[j, k] if self.n < 4 else table[k, j]

    def w(self, b):
        d, j, e = self.place(b)
        return self.ref["w"][j] if d == 0 else self.ref["wn"][self.weight_ways.index(d), e]

    def row(self, name, b):
        d, j, e = self.place(b)
        if d == 0:
            return self.spread(self.ref[name][j, 0:1, :])
        return self.spread(self.ref[name + "n"][self.degree_ways.index(d), e, 0:1, :])

    def f(self, b):
        d, j, e = self.place(b)
        if d == 0:
            return self.ref["f"][j]
        return self.ref["fn"][self.degree_ways.index(d), e].astype(F32)

    def table(self, name, b):
        d, j, _ = self.place(b)
        if d == 0:
            return self.ref[name][j : j + 1, :]
        return self.ref[name + "n"][self.weight_ways.index(d), j : j + 1, :]

    def owner(self, b):
        return self.spread(self.table("own", b) - self.ops.me)

    def invert(self):
        for at in range(len(self.degree_ways)):
            for e in range(self.m):
                self.ref["gin"][at, e] = DAMPING / self.ref["gn"][at, e]

    def make_onehots(self, reach):
        for b in range(-reach, self.n + reach):
            at = (b + reach) * self.bs
            self.put_hot(self.table("slot", b), slice(at, at + self.bs))

    def product(self, i, b):
        buf = self.ref[f"vb{i}"]
        offset = self.base - self.halo
        top = buf.shape[0] - 1
        picked = [
            buf[jnp.clip(self.column(b, k) - offset, 0, top)] for k in range(self.k)
        ]
        left = jnp.concatenate(picked, axis=1)
        return jnp.dot(left, self.w(b), preferred_element_type=F32) * self.scale

    def apply(self, i, blocks, body, size=6):
        blocks = list(blocks)
        for low in range(0, len(blocks), size):
            group = blocks[low : low + size]
            made = [self.product(i, b) for b in group]
            for b, product in zip(group, made):
                body(b, product)

    def start_blocks(self, low, high):
        for b in range(low, high):
            self.ref["vb0"][b + self.halo] = (self.row("gi", b) * self.f(b)).astype(BF16)

    def first_sweep(self, b, product):
        f, gi = self.f(b), self.row("gi", b)
        x0 = gi * f
        x = (1.0 - DAMPING) * x0 + gi * (f + product)
        self.ref["x"][b + self.halo] = x
        self.ref["vb1"][b + self.halo] = x.astype(BF16)

    def residual_of(self, b, product):
        return self.f(b) - self.row("g", b) * self.ref["x"][b + self.halo] + product

    def add_correction(self, reach):
        bs, r = self.bs, self.r
        corrections = {0: self.ref["uout"]}
        for at, d in enumerate(self.send_ways):
            corrections[d] = self.ref["uin"].at[at]
        for b in range(-reach, self.n + reach, 2):
            d, _, _ = self.place(b)
            left = jnp.concatenate([corrections[d + way][...] for way in (-1, 0, 1)], axis=0)
            at = (b + reach) * bs
            value = jnp.dot(left, self.ref["oh"][:, at : at + 2 * bs], preferred_element_type=F32)
            for half in range(2):
                part = value[:, half * bs : (half + 1) * bs]
                rel = self.owner(b + half) - d
                low, own, high = (part[way * r : (way + 1) * r] for way in range(3))
                add = jnp.where(rel == 0, own, jnp.where(rel < 0, low, high))
                x = self.ref["x"][b + half + self.halo] + add
                self.ref["x"][b + half + self.halo] = x
                self.ref["vb2"][b + half + self.halo] = x.astype(BF16)

    def sweep(self, i, out=None):
        def body(b, product):
            h = self.halo
            x = (1.0 - DAMPING) * self.ref["x"][b + h] + self.row("gi", b) * (self.f(b) + product)
            if out is None:
                self.ref["x"][b + h] = x
                self.ref[f"vb{i + 1}"][b + h] = x.astype(BF16)
            else:
                out(b, x)

        return body

    def clear_ends(self):
        for at, d in enumerate(self.weight_ways):

            @pl.when(jnp.logical_not(self.ops.has(d)))
            def _():
                self.ref["ownn"][at] = jnp.full(self.ref["ownn"].shape[1:], -8, jnp.int32)
                self.ref["slotn"][at] = jnp.zeros(self.ref["slotn"].shape[1:], jnp.int32)
                self.ref["wn"][at] = jnp.zeros(self.ref["wn"].shape[1:], BF16)
                columns = self.other_columns[at]
                for i in range(columns.shape[0]):
                    for j in range(columns.shape[1]):
                        columns[i, j] = 0

        for at, d in enumerate(self.degree_ways):

            @pl.when(jnp.logical_not(self.ops.has(d)))
            def _():
                self.ref["gn"][at] = jnp.ones(self.ref["gn"].shape[1:], F32)
                self.ref["fn"][at] = jnp.zeros(self.ref["fn"].shape[1:], self.ref["fn"].dtype)

        for at, d in enumerate(self.send_ways):

            @pl.when(jnp.logical_not(self.ops.has(d)))
            def _():
                self.ref["uin"][at] = jnp.zeros(self.ref["uin"].shape[1:], BF16)


class Second(Small):
    def __init__(self, *args):
        super().__init__(*args, 4, (-1, 1), (-1, 1), (-2, -1, 1, 2))
        ref, ops, n, h = self.ref, self.ops, self.n, self.halo
        vb, got = ref["vb1"], ref["vin"]
        own = lambda low, high: vb.at[h + low : h + high]
        self.halo_near = [
            ops.copy(own(n - 2, n), got.at[0, 2:4], 1), ops.copy(own(0, 2), got.at[1, 0:2], -1)
        ]
        self.halo_far = [
            ops.copy(own(n - 4, n - 2), got.at[0, 0:2], 1), ops.copy(own(2, 4), got.at[1, 2:4], -1)
        ]
        self.restrict_copies = [
            ops.copy(ref["rout"].at[1], ref["rin"].at[0], 1),
            ops.copy(ref["rout"].at[0], ref["rin"].at[1], -1),
        ]

    def residual(self, b, product):
        at = slice(b * self.bs, (b + 1) * self.bs)
        self.put_residual(at, self.residual_of(b, product), self.owner(b))

    def down(self, below, meanwhile):
        n, h, r, bs = self.n, self.halo, self.r, self.bs
        self.start_blocks(-2, n + 2)
        edges = [0, 1, n - 2, n - 1]
        self.apply(0, edges, self.first_sweep)
        start(self.halo_near)
        self.apply(0, range(2, n - 2), self.first_sweep)
        start(self.halo_far)
        meanwhile()
        self.apply(1, range(2, n - 2), self.residual)
        wait(self.halo_near)
        self.ref["vb1"][h - 2 : h] = self.ref["vin"][0, 2:4]
        self.ref["vb1"][h + n : h + n + 2] = self.ref["vin"][1, 0:2]
        self.apply(1, edges, self.residual)
        reach = 4
        own = slice(reach * bs, (reach + n) * bs)
        value = self.restricted(self.ref["res"][...], self.ref["oh"][:, own])
        for b in range(below.n):
            at = slice(b * bs, (b + 1) * bs)
            self.ref["rout"][0, b] = value[0:r, at].astype(BF16)
            self.ref["rout"][1, b] = value[2 * r : 3 * r, at].astype(BF16)
        start(self.restrict_copies)
        for b in range(below.n):
            self.ref["rown"][b] = value[r : 2 * r, b * bs : (b + 1) * bs]

    def received(self, below):
        wait(self.restrict_copies)
        got = self.ref["rin"]
        for b in range(below.n):
            f = self.ref["rown"][b] + got[0, b].astype(F32) + got[1, b].astype(F32)
            below.ref["f"][b] = f
            below.ref["fout"][b] = f.astype(BF16)

    def finish(self, out):
        n, h = self.n, self.halo
        wait(self.halo_far)
        for j in range(4):
            self.ref["x"][h - 4 + j] = self.ref["vin"][0, j].astype(F32)
            self.ref["x"][h + n + j] = self.ref["vin"][1, j].astype(F32)
        wait(self.sends)
        self.add_correction(4)
        for group in self.weights:
            wait(group)
        self.apply(2, range(-2, n + 2), self.sweep(2))
        self.apply(3, range(n), self.sweep(3, out))

    def clear_ends(self):
        super().clear_ends()
        for name in ("rin", "vin"):
            for at, d in ((0, -1), (1, 1)):

                @pl.when(jnp.logical_not(self.ops.has(d)))
                def _():
                    self.ref[name][at] = jnp.zeros(self.ref[name].shape[1:], BF16)


class Third(Small):
    def __init__(self, *args):
        super().__init__(*args, 6, (-2, -1, 1, 2), (-3, -2, -1, 1, 2, 3), (-3, -2, -1, 1, 2, 3))
        ref, ops = self.ref, self.ops
        self.sources = [
            ops.copy(ref["fout"], ref["fn"].at[at], -d)
            for at, d in self.far_first(self.degree_ways)
        ]

    def down(self, into):
        n, bs = self.n, self.bs
        wait(self.sources)
        self.start_blocks(-6, n + 6)
        for group in self.weights:
            wait(group)
        self.apply(0, range(-4, n + 4), self.first_sweep)

        def residual(b, product):
            res = self.residual_of(b, product)
            at = (b + 2) * bs
            kept = jnp.where(self.owner(b) == 0, res, jnp.zeros_like(res))
            self.ref["res"][:, at : at + bs] = kept.astype(BF16)

        self.apply(1, range(-2, n + 2), residual)
        near = slice(2 * bs, (n + 6) * bs)
        into(self.restricted(self.ref["res"][...], self.ref["oh"][:, near]))

    def finish(self, out):
        n = self.n
        wait(self.sends)
        self.add_correction(4)
        self.apply(2, range(-2, n + 2), self.sweep(2))
        self.apply(3, range(n), self.sweep(3, out))


LEVEL_HBM = ("w", "deg", "own", "slot")
SHARED = ("w", "deg", "own", "slot", "g", "gi", "x", "vb0", "vb1", "vb2", "vb3", "res", "oh", "uout", "uin")
FINE = SHARED + (
    "lo0", "lo1", "lo2", "lo3", "hi0", "hi1", "hi2", "hi3", "rout", "rin", "rown", "near", "far", "part",
)
SMALL = SHARED + ("f", "fn", "wn", "ownn", "slotn", "gn", "gin")
SECOND = SMALL + ("rout", "rin", "rown", "vin")
THIRD = SMALL + ("fout",)


def kernel(sizes, rhs_count, bs, k, *refs):
    refs = list(refs)
    take = lambda count: [refs.pop(0) for _ in range(count)]
    rhs_hbm, inverse_hbm = take(2)
    columns_hbm, hbm = [], []
    for _ in sizes:
        columns_hbm.append(refs.pop(0))
        hbm.append(dict(zip(LEVEL_HBM, take(4))))
    (out,) = take(1)
    scratch = [dict(zip(names, take(len(names)))) for names in (FINE, SECOND, THIRD)]
    columns = [take(1), take(3), take(5)]
    rhs, inverse, gathered = take(3)
    send, recv, gather_send, gather_recv, local = take(5)

    ops = Ops(send, recv)
    scratch[0]["f"] = rhs
    (n0, t0), (n1, t1), (n2, t2) = sizes
    fine = Fine(n0, t0, rhs_count, bs, k, scratch[0], columns[0][0], ops)
    second = Second(n1, t1, rhs_count, bs, k, scratch[1], columns[1], ops)
    third = Third(n2, t2, rhs_count, bs, k, scratch[2], columns[2], ops)
    levels = [fine, second, third]

    loads = []

    def load(src, dst):
        copy = pltpu.make_async_copy(src, dst, local.at[len(loads)])
        loads.append(copy)
        copy.start()
        return copy

    n = fine.n
    early = []
    for at in (slice(0, 2), slice(n - 2, n)):
        early.append(load(hbm[0]["w"].at[at], scratch[0]["w"].at[at]))
    early.append(load(hbm[0]["deg"], scratch[0]["deg"]))
    early.append(load(rhs_hbm, rhs))
    for level in range(3):
        early.append(load(columns_hbm[level], columns[level][0]))
    heavy = load(hbm[2]["w"], scratch[2]["w"])
    middle = load(hbm[0]["w"].at[2 : n - 2], scratch[0]["w"].at[2 : n - 2])
    later = [load(hbm[0][name], scratch[0][name]) for name in ("own", "slot")]
    for position in (1, 2):
        names = LEVEL_HBM[position - 1 :]
        later += [load(hbm[position][name], scratch[position][name]) for name in names]
    last = load(inverse_hbm, inverse)

    barrier = pltpu.get_barrier_semaphore()
    expected = ops.cols - 1
    for delta in (-3, -2, -1, 1, 2, 3):
        outside = ops.across(delta)
        pl.when(outside)(
            lambda: pl.semaphore_signal(
                barrier, inc=1, device_id=ops.peer(delta), device_id_type=MESH
            )
        )
        expected = expected + outside.astype(jnp.int32)
    for step in range(1, ops.cols):
        peer = lax.rem(ops.col + step, ops.cols)
        pl.semaphore_signal(barrier, inc=1, device_id=(ops.row, peer), device_id_type=MESH)
    for level in levels:
        level.clear_ends()
    for copy in early:
        copy.wait()

    def diagonal_and_start(b, total):
        fine.put_diagonal(b, total)
        fine.start_block(b)

    made = [fine.weight_sums(b) for b in fine.edges()]
    for b, total in zip(fine.edges(), made):
        diagonal_and_start(b, total)
    pl.semaphore_wait(barrier, expected)
    start(fine.halo[0])
    third_weights = Slots(third.weights, THIRD_SLOTS)
    second_weights = Slots(second.weights, SECOND_SLOTS)
    heavy.wait()
    third_weights.send()
    middle.wait()
    grouped(*fine.inner(), fine.weight_sums, diagonal_and_start)
    for copy in later:
        copy.wait()
    for level in (second, third):
        grouped(0, level.n, level.weight_sums, level.put_diagonal, 8)
    start(second.tables)
    loop(0, n, fine.make_onehot, 2)
    fine.apply(0, fine.first_sweep)
    start(fine.halo[1])
    third_weights.send()
    start(third.tables)
    fine.apply(1, fine.residual, fine.restrict_inner)
    fine.restrict()
    for level in (second, third):
        wait(level.tables)
        level.invert()
        level.make_onehots(4)
    fine.received(second)

    second.down(third, third_weights.send)
    third_weights.send()
    second_weights.send()
    second.received(third)
    start(third.sources)
    second_weights.send()

    def into_coarse(value):
        gathered[ops.col] = value.astype(BF16)

    third.down(into_coarse)

    sends = []
    for step in range(1, ops.cols):
        peer = lax.rem(ops.col + step, ops.cols)
        copy = pltpu.make_async_remote_copy(
            gathered.at[ops.col], gathered.at[ops.col],
            gather_send.at[step - 1], gather_recv.at[step - 1],
            device_id=(ops.row, peer), device_id_type=MESH,
        )
        copy.start()
        sends.append(copy)
    second_weights.send()
    last.wait()
    for step in range(1, ops.cols):
        source = lax.rem(ops.col + ops.cols - step, ops.cols)
        pltpu.make_async_remote_copy(
            gathered.at[source], gathered.at[source],
            gather_send.at[step - 1], gather_recv.at[step - 1],
            device_id=(ops.row, source), device_id_type=MESH,
        ).wait_recv()
    everything = jnp.concatenate([gathered[p] for p in range(ops.cols)], axis=1)
    solved = lax.dot_general(
        everything, inverse[...], (((1,), (1,)), ((), ())), preferred_element_type=F32
    )
    third.ref["uout"][...] = solved.astype(BF16)
    start(third.sends)
    second_weights.send()

    def into_coarse_vector(level):
        def put(b, x):
            level.ref["uout"][:, b * bs : (b + 1) * bs] = x.astype(BF16)

        return put

    third.finish(into_coarse_vector(second))
    start(second.sends)
    second.finish(into_coarse_vector(fine))
    fine.up(out)
    for copy in ops.copies:
        copy.drain()
    for copy in sends:
        copy.wait_send()


def on_device(
    right_sides,
    weights_fine, columns_fine, degree_fine, owners_fine, slots_fine,
    weights_second, columns_second, degree_second, owners_second, slots_second,
    weights_third, columns_third, degree_third, owners_third, slots_third,
    coarse_inverse,
):
    n0, r, bs = right_sides.shape
    n1, n2 = weights_second.shape[0], weights_third.shape[0]
    k = weights_fine.shape[1]
    c3, m3 = coarse_inverse.shape
    cols = lax.axis_size("col")
    sizes = ((n0, n1 * bs), (n1, n2 * bs), (n2, c3))
    merged = lambda w: w.reshape(w.shape[0], k * bs, bs)
    args = [right_sides, coarse_inverse]
    for w, c, d, o, s in (
        (weights_fine, columns_fine, degree_fine, owners_fine, slots_fine),
        (weights_second, columns_second, degree_second, owners_second, slots_second),
        (weights_third, columns_third, degree_third, owners_third, slots_third),
    ):
        args += [c.T if c.shape[0] >= 4 else c, merged(w), d, o, s]
    specs = [pl.BlockSpec(memory_space=pltpu.HBM)] * len(args)
    vmem = pltpu.VMEM
    vector = lambda *lead: vmem((*lead, r, bs), BF16)

    def shared(n, t, window, ways, res, hot):
        return [
            vmem((n, k * bs, bs), BF16),
            vmem((n, bs), F32),
            vmem((n, bs), jnp.int32),
            vmem((n, bs), jnp.int32),
            vmem((n, 8, bs), F32),
            vmem((n, 8, bs), F32),
            vmem((window, r, bs), F32),
            *[vector(window)] * 4,
            vmem((res[0] * r, res[1] * bs), BF16),
            vmem((t, hot * bs), F8),
            vmem((r, t), BF16),
            vmem((ways, r, t), BF16),
        ]

    def small(n, weights, degrees, source):
        m = min(n, 2)
        return [
            vmem((n, r, bs), F32),
            vmem((degrees, m, r, bs), source),
            vmem((weights, m, k * bs, bs), BF16),
            vmem((weights, n, bs), jnp.int32),
            vmem((weights, n, bs), jnp.int32),
            vmem((degrees, m, 8, bs), F32),
            vmem((degrees, m, 8, bs), F32),
        ]

    scratch = shared(n0, n1 * bs, n0, 2, (3, n0), n0)
    scratch += [vector(6)] * 8
    scratch += [vector(3, n1), vector(2, n1), vmem((n1, r, bs), F32), vector(2, 2), vector(2, 2)]
    scratch += [vmem((3 * r, n1 * bs), F32)]
    scratch += shared(n1, n2 * bs, n1 + 8, 4, (3, n1), n1 + 8)
    scratch += small(n1, 2, 2, F32)
    scratch += [vector(2, n2), vector(2, n2), vmem((n2, r, bs), F32), vector(2, 4)]
    scratch += shared(n2, c3, n2 + 12, 6, (1, n2 + 4), n2 + 8)
    scratch += small(n2, 4, 6, BF16)
    scratch += [vector(n2)]
    scratch += [pltpu.SMEM((k, n0), jnp.int32)]
    scratch += [pltpu.SMEM((k, n1), jnp.int32)] * 3
    scratch += [pltpu.SMEM((n2, k), jnp.int32)] * 5
    scratch += [
        vector(n0),
        vmem((c3, m3), BF16),
        vmem((cols, r, c3), BF16),
        pltpu.SemaphoreType.DMA((140,)),
        pltpu.SemaphoreType.DMA((140,)),
        pltpu.SemaphoreType.DMA((cols,)),
        pltpu.SemaphoreType.DMA((cols,)),
        pltpu.SemaphoreType.DMA((24,)),
    ]
    return pl.pallas_call(
        functools.partial(kernel, sizes, r, bs, k),
        out_shape=jax.ShapeDtypeStruct((n0, r, bs), F32),
        in_specs=specs,
        out_specs=pl.BlockSpec(memory_space=pltpu.VMEM),
        scratch_shapes=scratch,
        compiler_params=pltpu.CompilerParams(
            collective_id=0, has_side_effects=True, vmem_limit_bytes=48 * 1024 * 1024
        ),
        name="vcycle",
    )(*[pltpu.with_memory_space_constraint(a, pltpu.HBM) for a in args])


def solution(mesh):
    whole = ("row", "col")
    vector, matrix, table = P(whole, None, None), P(whole, None, None, None), P(whole, None)
    level = (matrix, table, table, table, table)
    return jax.shard_map(
        on_device,
        mesh=mesh,
        in_specs=(vector, *level, *level, *level, table),
        out_specs=vector,
        check_vma=False,
    )
```
